512 devices in a mesh: tile: 32 (over z, y_hi), col: 16 (over x, y_lo, core).
Axes of the slice: x: 4, y: 8 (y_hi: 4, y_lo: 2; y = y_hi * 2 + y_lo), z: 8, core: 2. Of those that a mesh axis runs over, the one named last changes fastest.
Arguments:
- latent: bfloat16 [32, 17, 4, 64, 256], P('tile', None, None, 'col'), may hold values from -20 to 20
- intersections: int32 [32], P('tile'), may hold values from 0 to 4, as said below
- norm_gain_one: float32 [256], replicated, may hold values from 0.5 to 1.5
- norm_shift_one: float32 [256], replicated, may hold values from -3 to 3
- weight_one: bfloat16 [3, 3, 3, 256, 256], P(None, None, None, 'col'), may hold values from -0.078125 to 0.078125
- norm_gain_two: float32 [256], replicated, may hold values from 0.5 to 1.5
- norm_shift_two: float32 [256], replicated, may hold values from -3 to 3
- weight_two: bfloat16 [3, 3, 3, 256, 256], P(None, None, None, 'col'), may hold values from -0.078125 to 0.078125
- conv_bias: float32 [256], replicated, may hold values from -1.8 to 1.8
Outputs:
- blended: bfloat16 [32, 17, 4, 64, 256], P('tile', None, None, 'col')
The draws below stay inside these ranges and needn't reach their ends.
Inputs may be any that keep to these rules, and one draw needn't show every extreme that they name: intersections[0] is 0 and every other entry is 1 to 4; some entry equals 4.
All inputs are finite; a program needn't handle non-finite values.
Results may differ from the reference program's by a relative error of at most 0.0055.
Values may be sent and summed in bfloat16 or wider, within the bound.
No kernel may reach another device: no remote copies, remote signals or barrier semaphores. Data moves between devices by JAX's collectives and lax.ppermute only.
A program may use at most 64 MiB of HBM per device.

```python
import jax
import jax.numpy as jnp
from jax import lax

C = 256
GROUPS = 32
FT = 17
OVMAX = 4
H = 4
TILES = 32
W = 64


def draw_latent(key, part):
    shape = (TILES, FT, H, W, C)
    column = jnp.arange(W, dtype=jnp.float32) / (W - 1)
    factor = 3.0 ** column
    base = jnp.clip(jax.random.normal(key, shape, jnp.float32), -6.0, 6.0)
    return (base * factor[:, None]).astype(jnp.bfloat16)


def draw_intersections(key, part):
    counts = jax.random.randint(key, (TILES,), 1, OVMAX + 1)
    chosen = jax.random.randint(jax.random.fold_in(key, 7), (), 1, TILES)
    places = jnp.arange(TILES, dtype=jnp.int32)
    counts = jnp.where(places == chosen, OVMAX, counts)
    counts = jnp.where(places == 0, 0, counts)
    return counts.astype(jnp.int32)


def steps_of(rng, shape, shards, least, high):
    factor_of = 1.0
    for dim, blocks in shards:
        draws = jax.random.uniform(jax.random.fold_in(jax.random.fold_in(rng, 6), dim), (blocks,), jnp.float32, least / len(shards), high / len(shards))
        factor_of = factor_of * jnp.repeat(jnp.exp(draws), shape[dim] // blocks).reshape((-1,) + (1,) * (len(shape) - 1 - dim))
    return factor_of


def gaussian(stream_key, dims, scale, bound, cuts=(), kind=jnp.bfloat16):
    factor_of = steps_of(stream_key, dims, cuts, -0.22, 0.18) if cuts else 1.0
    array = jax.random.normal(stream_key, dims, jnp.float32) * scale * factor_of
    return jnp.minimum(jnp.maximum(array, -bound), bound).astype(kind)


def setup_inputs(seed: int = 0) -> dict:
    splits = jax.random.split(jax.random.key(seed), 10)
    return {
        "latent": draw_latent(jax.random.fold_in(splits[9], 71), 0),
        "intersections": draw_intersections(jax.random.fold_in(splits[9], 71), 0),
        "norm_gain_one": jnp.clip(1.0 + 0.1 * jax.random.normal(splits[2], (C,), jnp.float32), 0.5, 1.5),
        "norm_shift_one": gaussian(splits[3], (C,), 0.5, 3.0, (), jnp.float32),
        "weight_one": gaussian(splits[4], (3, 3, 3, C, C), (27 * C) ** -0.5, 0.078125, ((3, 16),)),
        "norm_gain_two": jnp.clip(1.0 + 0.1 * jax.random.normal(splits[5], (C,), jnp.float32), 0.5, 1.5),
        "norm_shift_two": gaussian(splits[6], (C,), 0.5, 3.0, (), jnp.float32),
        "weight_two": gaussian(splits[7], (3, 3, 3, C, C), (27 * C) ** -0.5, 0.078125, ((3, 16),)),
        "conv_bias": gaussian(splits[8], (C,), 0.3, 1.8, (), jnp.float32),
    }


epsilon = 1e-06

def norm_silu(values, gain, shift):
    frames, height, width, channels = values.shape
    per_group = channels // GROUPS
    grouped = values.reshape(frames, height, width, GROUPS, per_group)
    group_mean = lax.optimization_barrier(jnp.mean(grouped, axis=(0, 1, 2, 4)))
    centred = grouped - group_mean[:, None]
    spread = lax.optimization_barrier(jnp.mean(centred * centred, axis=(0, 1, 2, 4)))
    normed = centred * lax.rsqrt(spread + epsilon)[:, None]
    normed = normed.reshape(values.shape) * gain + shift
    return jax.nn.silu(normed).astype(jnp.bfloat16)

def conv_taps(padded, kernel):
    frames = padded.shape[0]
    height = padded.shape[1]
    out_width = padded.shape[2] - 2
    channels = padded.shape[3]
    outputs = kernel.shape[4]
    padded = jnp.pad(padded, ((2, 0), (1, 1), (0, 0), (0, 0)))
    running = jnp.zeros((frames * height * out_width, outputs), jnp.float32)
    for tap_t in range(3):
        for tap_h in range(3):
            for tap_w in range(3):
                window = padded[tap_t:tap_t + frames, tap_h:tap_h + height, tap_w:tap_w + out_width]
                running = running + jnp.dot(window.reshape(-1, channels), kernel[tap_t, tap_h, tap_w], preferred_element_type=jnp.float32)
    return running.reshape(frames, height, out_width, outputs)

def reference(latent, intersections, norm_gain_one, norm_shift_one, weight_one, norm_gain_two, norm_shift_two, weight_two, conv_bias):

    def decode_tile(source):
        latent_full = source.astype(jnp.float32)
        act_one = norm_silu(latent_full, norm_gain_one, norm_shift_one)
        padded = jnp.pad(act_one, ((0, 0), (0, 0), (1, 1), (0, 0)))
        hidden = conv_taps(padded, weight_one).astype(jnp.bfloat16)
        act_two = norm_silu(hidden.astype(jnp.float32), norm_gain_two, norm_shift_two)
        padded = jnp.pad(act_two, ((0, 0), (0, 0), (1, 1), (0, 0)))
        branch = conv_taps(padded, weight_two) + conv_bias
        return (latent_full + branch).astype(jnp.bfloat16)
    decoded = lax.map(decode_tile, latent)
    frames = decoded.shape[1]
    prev_tails = jnp.concatenate([jnp.zeros_like(decoded[:1, :OVMAX]), decoded[:-1, frames - OVMAX:]], axis=0)
    extended = jnp.concatenate([prev_tails, jnp.zeros_like(prev_tails)], axis=1)

    def align(ext_tile, shared):
        return lax.dynamic_slice_in_dim(ext_tile, (OVMAX - shared).astype(jnp.int32), OVMAX, 0)
    aligned = jax.vmap(align)(extended, intersections)
    position = jnp.arange(OVMAX, dtype=jnp.int32)
    own_share = (position[None, :] + 1).astype(jnp.float32) / (intersections[:, None] + 1).astype(jnp.float32)
    own_share = own_share[:, :, None, None, None]
    head = decoded[:, :OVMAX].astype(jnp.float32)
    active = position[None, :, None, None, None] < intersections[:, None, None, None, None]
    mixed = jnp.where(active, own_share * head + (1.0 - own_share) * aligned.astype(jnp.float32), head)
    return jnp.concatenate([mixed.astype(jnp.bfloat16), decoded[:, OVMAX:]], axis=1)
```

```python
import jax
import jax.numpy as jnp
from jax import lax
from jax.experimental import pallas as pl
from jax.experimental.pallas import tpu as pltpu
from jax.sharding import Mesh
from jax.sharding import PartitionSpec as P

GROUPS = 32
OVMAX = 4
epsilon = 1e-06
F32, BF16 = jnp.float32, jnp.bfloat16

COL = ("x", "yl", "core")
JAX_ = ("yl", "core")
TILE = ("z", "yh")
T, H, W, C = 17, 4, 64, 256
ROW = 24
PARAMS = pltpu.CompilerParams(vmem_limit_bytes=48 * 1024 * 1024)


def whole():
    return pl.BlockSpec(memory_space=pltpu.VMEM)


def call(kernel, inputs, out_shape, scratch=(), cost=None):
    return pl.pallas_call(
        kernel,
        out_shape=out_shape,
        in_specs=[whole()] * len(inputs),
        out_specs=jax.tree.map(lambda _: whole(), out_shape),
        scratch_shapes=list(scratch),
        compiler_params=PARAMS,
        cost_estimate=cost,
    )(*inputs)


def cost(us):
    return pl.CostEstimate(flops=int(us * 4e8), bytes_accessed=1 << 20, transcendentals=0)


def lanes(shape):
    return lax.broadcasted_iota(jnp.int32, shape, len(shape) - 1)


def rows(shape):
    return lax.broadcasted_iota(jnp.int32, shape, len(shape) - 2)


def split3(value):
    high = value.astype(BF16)
    rest = value - high.astype(F32)
    middle = rest.astype(BF16)
    return high, middle, (rest - middle.astype(F32)).astype(BF16)


def group_sum(value):
    lane, width = lanes(value.shape), value.shape[1]
    for k in (1, 2, 4):
        up, down = pltpu.roll(value, k, 1), pltpu.roll(value, width - k, 1)
        value = value + jnp.where((lane & k) != 0, up, down)
    return value


def group_stats(total, squares):
    members = T * H * W * (C // GROUPS)
    mean = group_sum(total) / members
    spread = jnp.maximum(group_sum(squares) / members - mean * mean, 0.0)
    return mean, lax.rsqrt(spread + epsilon)


def silu(v):
    return v * (0.5 * jnp.tanh(0.5 * v) + 0.5)


def pack_kernel(w_ref, out_ref):
    row, col = rows((C, C)), lanes((C, C))
    source = 64 * ((col // 16) % 4) + 16 * (col // 64) + col % 16
    swapped = col ^ 64
    other = 64 * ((swapped // 16) % 4) + 16 * (swapped // 64) + swapped % 16
    left = lanes((16, 128)) < 64
    w = w_ref[...].reshape(27 * 16, C)
    same = jnp.dot(w, (row == source).astype(BF16), preferred_element_type=F32)
    swap = jnp.dot(w, (row == other).astype(BF16), preferred_element_type=F32)

    def block(array, k, dw, j):
        dt, dh = k % 3, k // 3
        at = ((dt * 3 + dh) * 3 + dw) * 16
        return array[at : at + 16, 128 * (j // 2) : 128 * (j // 2) + 128]

    for j in range(4):
        first, second = (same, swap) if j % 2 == 0 else (swap, same)
        for m in range(14):
            if m < 9:
                a, b = block(first, m, 0, j), block(second, m, 1, j)
            else:
                a = block(first, m - 9, 2, j)
                b = block(second, m - 4, 2, j) if m < 13 else jnp.zeros((16, 128), F32)
            tile = jnp.where(left, a, b).astype(BF16)
            for x in range(4):
                out_ref[4 * x + j, m] = tile


def edge_kernel(l_ref, out_ref):
    me = lax.axis_index("x")
    total, squares = jnp.zeros((4, C), F32), jnp.zeros((4, C), F32)
    for q in range(4):
        v = l_ref[q].astype(F32)
        total += jnp.sum(v, axis=(0, 1))
        squares += jnp.sum(v * v, axis=(0, 1))
    total = jnp.sum(total, axis=0, keepdims=True)
    squares = jnp.sum(squares, axis=0, keepdims=True)
    zero = jnp.zeros((1, C), F32)
    for half, value in ((0, total), (1, squares)):
        pieces = [p.astype(F32) for p in split3(value)]
        slab = jnp.concatenate(pieces + [zero], axis=0).astype(BF16)
        for d in range(4):
            out_ref[d, T, half] = slab
    right, left = lax.rem(me + 1, 4), lax.rem(me + 3, 4)

    def frame(t, _):
        for pair in range(2):
            ends = [l_ref[3, t, 2 * pair + i].astype(F32)[2:4] for i in range(2)]
            out_ref[right, t, pair] = jnp.concatenate(ends, axis=0).astype(BF16)
            starts = [l_ref[0, t, 2 * pair + i].astype(F32)[0:2] for i in range(2)]
            out_ref[left, t, pair] = jnp.concatenate(starts, axis=0).astype(BF16)
        return 0

    lax.fori_loop(0, T, frame, 0)


def conv_one_kernel(l_ref, e_ref, w_ref, gain_ref, shift_ref, hid_ref, st_ref, act, wm):
    me = lax.axis_index("x")
    left = lanes((16, 128)) < 64
    nothing = jnp.zeros((16, 128), BF16)
    for p in range(16):
        for k in range(9):
            wm[k, 16 * p : 16 * p + 16, 0:128] = w_ref[p, k]
            if k < 5:
                last = jnp.where(left, w_ref[p, 9 + k], nothing)
            else:
                last = jnp.where(left, nothing, w_ref[p, 4 + k])
            wm[k, 16 * p : 16 * p + 16, 128:256] = last
    total, squares = jnp.zeros((4, C), F32), jnp.zeros((4, C), F32)
    for s in range(4):
        total += e_ref[s, T, 0].astype(F32)
        squares += e_ref[s, T, 1].astype(F32)
    total = jnp.broadcast_to(jnp.sum(total, axis=0, keepdims=True), (8, C))
    squares = jnp.broadcast_to(jnp.sum(squares, axis=0, keepdims=True), (8, C))
    mean, inv = group_stats(total, squares)
    scale = inv * gain_ref[...]
    mean, scale = mean[0:1], scale[0:1]
    shift = shift_ref[...]
    before, after = lax.rem(me + 3, 4), lax.rem(me + 1, 4)
    row = rows((ROW, C))
    inside = (row >= jnp.where(me == 0, 4, 0)) & (row < jnp.where(me == 3, 20, ROW))
    act[:, 0:2] = jnp.zeros((4, 2, ROW, C), BF16)

    def frame(t, _):
        for h in range(4):
            lo = e_ref[before, t, h // 2].astype(F32)
            hi = e_ref[after, t, h // 2].astype(F32)
            if h % 2 == 0:
                lo = jnp.concatenate([lo[2:4], lo[0:2]], axis=0)
            else:
                hi = jnp.concatenate([hi[2:4], hi[0:2]], axis=0)
            own = [l_ref[q, t, h].astype(F32) for q in range(4)]
            v = jnp.concatenate([lo, *own, hi], axis=0)
            y = silu((v - mean) * scale + shift)
            act[h, t + 2] = jnp.where(inside, y, 0.0).astype(BF16)
        return 0

    lax.fori_loop(0, T, frame, 0)

    size = T * ROW
    lane = lanes((size, 128))
    place = rows((size, 128)) % ROW
    own = (place >= 4) & (place < 20)
    s1, s2 = jnp.zeros((1, 128), F32), jnp.zeros((1, 128), F32)
    for h in range(4):
        taps = [dh for dh in range(3) if 0 <= h + dh - 1 < 4]
        lhs = jnp.concatenate(
            [act[h + dh - 1, dt : dt + T].reshape(size, C) for dh in taps for dt in range(3)], axis=1
        )
        rhs = wm[3 * taps[0] : 3 * taps[-1] + 3].reshape(-1, C)
        y = jnp.dot(lhs, rhs, preferred_element_type=F32)
        y0, y1 = y[:, 0:128], y[:, 128:256]
        z = jnp.where(lane < 64, pltpu.roll(y0, 1, 0), y0) + pltpu.roll(y1, size - 1, 0)
        hidden = (z + pltpu.roll(z, 64, 1)).astype(BF16)
        hid_ref[h] = hidden.reshape(T, ROW, 128)
        counted = jnp.where(own, hidden.astype(F32), 0.0)
        s1 += jnp.sum(counted, axis=0, keepdims=True)
        s2 += jnp.sum(counted * counted, axis=0, keepdims=True)
    stats = jnp.concatenate([s1, s2, jnp.zeros((6, 128), F32)], axis=0)
    for d in range(4):
        st_ref[d] = stats


def conv_two_kernel(hid_ref, st_ref, w_ref, gain_ref, shift_ref, part_ref, act, wm):
    me = lax.axis_index("x")
    j = 2 * lax.axis_index("yl") + lax.axis_index("core")
    for dh in range(3):
        for dt in range(3):
            k = 3 * dh + dt
            for dw in range(3):
                for x in range(4):
                    at = 64 * dw + 16 * x
                    wm[k, at : at + 16] = w_ref[x, dt, dh, dw]
            wm[k, 192:256] = jnp.zeros((64, C), BF16)
    stats = st_ref[0] + st_ref[1] + st_ref[2] + st_ref[3]
    mean, inv = group_stats(
        jnp.broadcast_to(stats[0:1], (8, 128)), jnp.broadcast_to(stats[1:2], (8, 128))
    )
    row, lane = rows((C, 128)), lanes((C, 128))
    mine = (row == 64 * ((lane // 16) % 4) + 16 * j + lane % 16).astype(F32)
    pick = lambda ref: jnp.dot(
        jnp.broadcast_to(ref[...], (8, C)), mine, precision=lax.Precision.HIGHEST,
        preferred_element_type=F32,
    )
    scale = (inv * pick(gain_ref))[0:1]
    shift = pick(shift_ref)[0:1]
    mean = mean[0:1]
    row = rows((ROW, 128))
    inside = (row >= jnp.where(me == 0, 4, 0)) & (row < jnp.where(me == 3, 20, ROW))
    left = lanes((16, 128)) < 64
    act[:, 0:2] = jnp.zeros((4, 2, 16, C), BF16)

    def frame(t, _):
        for h in range(4):
            v = hid_ref[h, t].astype(F32)
            y = silu((v - mean) * scale + shift)
            y = jnp.where(inside, y, 0.0)
            a0, a1, a2 = (pltpu.roll(y, ROW - 3 - dw, 0)[0:16] for dw in range(3))
            act[h, t + 2, :, 0:128] = jnp.where(left, a0, a1).astype(BF16)
            act[h, t + 2, :, 128:256] = jnp.where(left, a2, 0.0).astype(BF16)
        return 0

    lax.fori_loop(0, T, frame, 0)
    for h in range(4):
        taps = [dh for dh in range(3) if 0 <= h + dh - 1 < 4]
        lhs = jnp.concatenate(
            [act[h + dh - 1, dt : dt + T].reshape(T * 16, C) for dh in taps for dt in range(3)], axis=1
        )
        rhs = wm[3 * taps[0] : 3 * taps[-1] + 3].reshape(-1, C)
        y = jnp.dot(lhs, rhs, preferred_element_type=F32).reshape(T, 16, C)
        for d in range(4):
            part_ref[d, :, h] = y[:, 4 * d : 4 * d + 4].astype(BF16)


def decode(part_ref, latent_ref, bias, t):
    branch = part_ref[0, t].astype(F32)
    for s in range(1, 4):
        branch = branch + part_ref[s, t].astype(F32)
    return (latent_ref[t].astype(F32) + (branch + bias)).astype(BF16)


def tail_kernel(part_ref, latent_ref, bias_ref, tail_ref):
    for i in range(OVMAX):
        tail_ref[i] = decode(part_ref, latent_ref, bias_ref[...], T - OVMAX + i)


def blend_kernel(shared_ref, part_ref, latent_ref, bias_ref, received_ref, out_ref):
    shared = shared_ref[0]
    bias = bias_ref[...]
    for t in range(T):
        own = decode(part_ref, latent_ref, bias, t)
        if t < OVMAX:
            source = jnp.clip(OVMAX - shared + t, 0, OVMAX - 1)
            other = received_ref[source].astype(F32)
            top = jnp.full((1, 1, C), t + 1, jnp.int32).astype(F32)
            share = top / jnp.full((1, 1, C), shared + 1, jnp.int32).astype(F32)
            head = own.astype(F32)
            mixed = share * head + (1.0 - share) * other
            active = jnp.full((1, 1, C), shared, jnp.int32) > t
            own = jnp.where(active, mixed, head).astype(BF16)
        out_ref[t] = own


def exchange(array, axis):
    return lax.all_to_all(array, axis, split_axis=0, concat_axis=0, tiled=True)


def shards(latent, intersections, gain_one, shift_one, weight_one, gain_two, shift_two, weight_two, bias):
    source = latent[0]
    flat = lambda v: v.reshape(1, C)
    sds = jax.ShapeDtypeStruct
    packed = call(pack_kernel, (weight_one,), sds((16, 14, 16, 128), BF16), cost=cost(1))
    kernel_one = exchange(packed, COL)
    wide = lax.all_gather(source, JAX_, axis=0, tiled=False)
    edges = call(edge_kernel, (wide,), sds((4, T + 1, 2, 4, C), BF16), cost=cost(1))
    edges = exchange(edges, "x")
    kernel_two = exchange(jnp.broadcast_to(weight_two[None], (4, *weight_two.shape)), "x")
    hidden, stats = call(
        conv_one_kernel,
        (wide, edges, kernel_one, flat(gain_one), flat(shift_one)),
        (sds((4, T, ROW, 128), BF16), sds((4, 8, 128), F32)),
        (pltpu.VMEM((4, T + 2, ROW, C), BF16), pltpu.VMEM((9, C, C), BF16)),
        cost=cost(4),
    )
    stats = exchange(stats, "x")
    part = call(
        conv_two_kernel,
        (hidden, stats, kernel_two, flat(gain_two), flat(shift_two)),
        sds((4, T, 4, 4, C), BF16),
        (pltpu.VMEM((4, T + 2, 16, C), BF16), pltpu.VMEM((9, C, C), BF16)),
        cost=cost(4),
    )
    part = exchange(part, JAX_)
    tail = call(tail_kernel, (part, source, flat(bias)), sds((OVMAX, 4, 4, C), BF16), cost=cost(1))
    tiles = lax.axis_size(TILE)
    received = lax.ppermute(tail, TILE, [(i, i + 1) for i in range(tiles - 1)])
    out = pl.pallas_call(
        blend_kernel,
        out_shape=sds((T, 4, 4, C), BF16),
        in_specs=[pl.BlockSpec(memory_space=pltpu.SMEM)] + [whole()] * 4,
        out_specs=whole(),
        compiler_params=PARAMS,
        cost_estimate=cost(1),
    )(intersections, part, source, flat(bias), received)
    return out[None]


def solution(mesh):
    wide = Mesh(mesh.devices.reshape(8, 4, 4, 2, 2), ("z", "yh", "x", "yl", "core"))
    image = P(TILE, None, None, COL, None)
    kernel = P(None, None, None, COL, None)
    in_specs = (image, P(TILE), P(), P(), kernel, P(), P(), kernel, P())
    return jax.shard_map(shards, mesh=wide, in_specs=in_specs, out_specs=image, check_vma=False)
```

```python
import jax
import jax.numpy as jnp
from jax import lax
from jax.experimental import pallas as pl
from jax.experimental.pallas import tpu as pltpu
from jax.sharding import Mesh
from jax.sharding import PartitionSpec as P

GROUPS = 32
OVMAX = 4
epsilon = 1e-06
F32, BF16 = jnp.float32, jnp.bfloat16

COL = ("x", "yl", "core")
JAX_ = ("yl", "core")
TILE = ("z", "yh")
T, H, W, C = 17, 4, 64, 256
ROW = 24
PARAMS = pltpu.CompilerParams(vmem_limit_bytes=48 * 1024 * 1024)


def whole():
    return pl.BlockSpec(memory_space=pltpu.VMEM)


def call(kernel, inputs, out_shape, scratch=(), cost=None):
    return pl.pallas_call(
        kernel,
        out_shape=out_shape,
        in_specs=[whole()] * len(inputs),
        out_specs=jax.tree.map(lambda _: whole(), out_shape),
        scratch_shapes=list(scratch),
        compiler_params=PARAMS,
        cost_estimate=cost,
    )(*inputs)


def cost(us):
    return pl.CostEstimate(flops=int(us * 4e8), bytes_accessed=1 << 20, transcendentals=0)


def lanes(shape):
    return lax.broadcasted_iota(jnp.int32, shape, len(shape) - 1)


def rows(shape):
    return lax.broadcasted_iota(jnp.int32, shape, len(shape) - 2)


def split3(value):
    high = value.astype(BF16)
    rest = value - high.astype(F32)
    middle = rest.astype(BF16)
    return high, middle, (rest - middle.astype(F32)).astype(BF16)


def group_sum(value):
    lane, width = lanes(value.shape), value.shape[1]
    for k in (1, 2, 4):
        up, down = pltpu.roll(value, k, 1), pltpu.roll(value, width - k, 1)
        value = value + jnp.where((lane & k) != 0, up, down)
    return value


def group_stats(total, squares):
    members = T * H * W * (C // GROUPS)
    mean = group_sum(total) / members
    spread = jnp.maximum(group_sum(squares) / members - mean * mean, 0.0)
    return mean, lax.rsqrt(spread + epsilon)


def silu(v):
    return v * (0.5 * jnp.tanh(0.5 * v) + 0.5)


def pack_kernel(w_ref, latent_ref, g1_ref, s1_ref, g2_ref, s2_ref, b_ref, out_ref, edge_ref, vec_ref):
    j = 2 * lax.axis_index("yl") + lax.axis_index("core")
    for i, ref in enumerate((g1_ref, s1_ref, g2_ref, s2_ref, b_ref)):
        vec_ref[i : i + 1] = ref[...]
    vec_ref[5:8] = jnp.zeros((3, C), F32)
    total, squares = jnp.zeros((4, C), F32), jnp.zeros((4, C), F32)
    first = jnp.full((2, C), j, jnp.int32) == 0
    for t in range(T):
        ends = []
        for h in range(H):
            v = latent_ref[t, h].astype(F32)
            total += v
            squares += v * v
            ends.append(jnp.where(first, v[0:2], v[2:4]))
        for pair in range(2):
            edge_ref[t, pair] = jnp.concatenate(ends[2 * pair : 2 * pair + 2], axis=0).astype(BF16)
    pieces = []
    for value in (total, squares):
        for piece in split3(jnp.sum(value, axis=0, keepdims=True)):
            piece = piece.astype(F32)
            pieces += [piece[:, 0:128], piece[:, 128:256]]
    sums = jnp.concatenate(pieces + [jnp.zeros((4, 128), F32)], axis=0).astype(BF16)
    for d in range(16):
        out_ref[d, 14] = sums
    row, col = rows((C, C)), lanes((C, C))
    source = 64 * ((col // 16) % 4) + 16 * (col // 64) + col % 16
    swapped = col ^ 64
    other = 64 * ((swapped // 16) % 4) + 16 * (swapped // 64) + swapped % 16
    left = lanes((16, 128)) < 64
    w = w_ref[...].reshape(27 * 16, C)
    same = jnp.dot(w, (row == source).astype(BF16), preferred_element_type=F32)
    swap = jnp.dot(w, (row == other).astype(BF16), preferred_element_type=F32)

    def block(array, k, dw, j):
        dt, dh = k % 3, k // 3
        at = ((dt * 3 + dh) * 3 + dw) * 16
        return array[at : at + 16, 128 * (j // 2) : 128 * (j // 2) + 128]

    for j in range(4):
        first, second = (same, swap) if j % 2 == 0 else (swap, same)
        for m in range(14):
            if m < 9:
                a, b = block(first, m, 0, j), block(second, m, 1, j)
            else:
                a = block(first, m - 9, 2, j)
                b = block(second, m - 4, 2, j) if m < 13 else jnp.zeros((16, 128), F32)
            tile = jnp.where(left, a, b).astype(BF16)
            for x in range(4):
                out_ref[4 * x + j, m] = tile


def join_kernel(latent_ref, edge_ref, out_ref):
    out_ref[:, 0:4] = latent_ref[...]
    out_ref[:, 4:6] = edge_ref[...]


def copies_kernel(w_ref, out_ref):
    for d in range(4):
        out_ref[d] = w_ref[...]


def conv_one_kernel(l_ref, w_ref, vec_ref, hid_ref, st_ref, act, wm):
    me = lax.axis_index("x")
    left = lanes((16, 128)) < 64
    nothing = jnp.zeros((16, 128), BF16)
    for p in range(16):
        for k in range(9):
            wm[k, 16 * p : 16 * p + 16, 0:128] = w_ref[p, k]
            if k < 5:
                last = jnp.where(left, w_ref[p, 9 + k], nothing)
            else:
                last = jnp.where(left, nothing, w_ref[p, 4 + k])
            wm[k, 16 * p : 16 * p + 16, 128:256] = last
    sums = sum(w_ref[p, 14].astype(F32) for p in range(16))
    joined = lambda i: jnp.concatenate(
        [sums[i + k : i + k + 1] + sums[i + k + 2 : i + k + 3] + sums[i + k + 4 : i + k + 5] for k in range(2)],
        axis=1,
    )
    total = jnp.broadcast_to(joined(0), (8, C))
    squares = jnp.broadcast_to(joined(6), (8, C))
    mean, inv = group_stats(total, squares)
    scale = inv * vec_ref[0:1]
    mean, scale = mean[0:1], scale[0:1]
    shift = vec_ref[1:2]
    row = rows((ROW, C))
    inside = (row >= jnp.where(me == 0, 4, 0)) & (row < jnp.where(me == 3, 20, ROW))
    act[:, 0:2] = jnp.zeros((4, 2, ROW, C), BF16)

    def frame(t, _):
        for h in range(4):
            lo = l_ref[0, t, 4 + h // 2].astype(F32)
            hi = l_ref[3, t, 4 + h // 2].astype(F32)
            if h % 2 == 0:
                lo = jnp.concatenate([lo[2:4], lo[0:2]], axis=0)
            else:
                hi = jnp.concatenate([hi[2:4], hi[0:2]], axis=0)
            own = [l_ref[q, t, h].astype(F32) for q in range(4)]
            v = jnp.concatenate([lo, *own, hi], axis=0)
            y = silu((v - mean) * scale + shift)
            act[h, t + 2] = jnp.where(inside, y, 0.0).astype(BF16)
        return 0

    lax.fori_loop(0, T, frame, 0)

    size = T * ROW
    lane = lanes((size, 128))
    place = rows((size, 128)) % ROW
    own = (place >= 4) & (place < 20)
    s1, s2 = jnp.zeros((1, 128), F32), jnp.zeros((1, 128), F32)
    for h in range(4):
        taps = [dh for dh in range(3) if 0 <= h + dh - 1 < 4]
        lhs = jnp.concatenate(
            [act[h + dh - 1, dt : dt + T].reshape(size, C) for dh in taps for dt in range(3)], axis=1
        )
        rhs = wm[3 * taps[0] : 3 * taps[-1] + 3].reshape(-1, C)
        y = jnp.dot(lhs, rhs, preferred_element_type=F32)
        y0, y1 = y[:, 0:128], y[:, 128:256]
        z = jnp.where(lane < 64, pltpu.roll(y0, 1, 0), y0) + pltpu.roll(y1, size - 1, 0)
        hidden = (z + pltpu.roll(z, 64, 1)).astype(BF16)
        hid_ref[h] = hidden.reshape(T, ROW, 128)
        counted = jnp.where(own, hidden.astype(F32), 0.0)
        s1 += jnp.sum(counted, axis=0, keepdims=True)
        s2 += jnp.sum(counted * counted, axis=0, keepdims=True)
    stats = jnp.concatenate([s1, s2, jnp.zeros((6, 128), F32)], axis=0)
    st_ref[...] = stats


def conv_two_kernel(hid_ref, st_ref, w_ref, vec_ref, part_ref, act, wm):
    me = lax.axis_index("x")
    j = 2 * lax.axis_index("yl") + lax.axis_index("core")
    for dh in range(3):
        for dt in range(3):
            k = 3 * dh + dt
            for dw in range(3):
                for x in range(4):
                    at = 64 * dw + 16 * x
                    wm[k, at : at + 16] = w_ref[x, dt, dh, dw]
            wm[k, 192:256] = jnp.zeros((64, C), BF16)
    stats = st_ref[...]
    mean, inv = group_stats(
        jnp.broadcast_to(stats[0:1], (8, 128)), jnp.broadcast_to(stats[1:2], (8, 128))
    )
    row, lane = rows((C, 128)), lanes((C, 128))
    mine = (row == 64 * ((lane // 16) % 4) + 16 * j + lane % 16).astype(F32)
    picked = jnp.dot(vec_ref[...], mine, precision=lax.Precision.HIGHEST, preferred_element_type=F32)
    scale, shift = inv[0:1] * picked[2:3], picked[3:4]
    mean = mean[0:1]
    row = rows((ROW, 128))
    inside = (row >= jnp.where(me == 0, 4, 0)) & (row < jnp.where(me == 3, 20, ROW))
    left = lanes((16, 128)) < 64
    act[:, 0:2] = jnp.zeros((4, 2, 16, C), BF16)

    def frame(t, _):
        for h in range(4):
            v = hid_ref[h, t].astype(F32)
            y = silu((v - mean) * scale + shift)
            y = jnp.where(inside, y, 0.0)
            a0, a1, a2 = (pltpu.roll(y, ROW - 3 - dw, 0)[0:16] for dw in range(3))
            act[h, t + 2, :, 0:128] = jnp.where(left, a0, a1).astype(BF16)
            act[h, t + 2, :, 128:256] = jnp.where(left, a2, 0.0).astype(BF16)
        return 0

    lax.fori_loop(0, T, frame, 0)
    for h in range(4):
        taps = [dh for dh in range(3) if 0 <= h + dh - 1 < 4]
        lhs = jnp.concatenate(
            [act[h + dh - 1, dt : dt + T].reshape(T * 16, C) for dh in taps for dt in range(3)], axis=1
        )
        rhs = wm[3 * taps[0] : 3 * taps[-1] + 3].reshape(-1, C)
        y = jnp.dot(lhs, rhs, preferred_element_type=F32).reshape(T, 16, C)
        for d in range(4):
            part_ref[d, :, h] = y[:, 4 * d : 4 * d + 4].astype(BF16)


def decode(part_ref, at, latent, bias):
    branch = part_ref[0, at].astype(F32)
    for q in range(1, 4):
        branch = branch + part_ref[q, at].astype(F32)
    return (latent.astype(F32) + (branch + bias)).astype(BF16)


def tail_kernel(part_ref, latent_ref, vec_ref, tail_ref):
    for i in range(OVMAX):
        tail_ref[i] = decode(part_ref, T - OVMAX + i, latent_ref[T - OVMAX + i], vec_ref[4:5])


def blend_kernel(shared_ref, main_ref, tail_ref, latent_ref, vec_ref, received_ref, out_ref):
    shared = shared_ref[0]
    bias = vec_ref[4:5]
    for t in range(T):
        if t >= T - OVMAX:
            out_ref[t] = tail_ref[t - T + OVMAX]
            continue
        own = decode(main_ref, t, latent_ref[t], bias)
        if t < OVMAX:
            source = jnp.clip(OVMAX - shared + t, 0, OVMAX - 1)
            other = received_ref[source].astype(F32)
            top = jnp.full((1, 1, C), t + 1, jnp.int32).astype(F32)
            share = top / jnp.full((1, 1, C), shared + 1, jnp.int32).astype(F32)
            head = own.astype(F32)
            mixed = share * head + (1.0 - share) * other
            active = jnp.full((1, 1, C), shared, jnp.int32) > t
            own = jnp.where(active, mixed, head).astype(BF16)
        out_ref[t] = own


def exchange(array, axis):
    return lax.all_to_all(array, axis, split_axis=0, concat_axis=0, tiled=True)


def block(latent, intersections, gain_one, shift_one, weight_one, gain_two, shift_two, weight_two, bias):
    source = latent[0]
    flat = lambda v: v.reshape(1, C)
    sds = jax.ShapeDtypeStruct
    vectors = tuple(flat(v) for v in (gain_one, shift_one, gain_two, shift_two, bias))
    packed, edge, vec = call(
        pack_kernel,
        (weight_one, source, *vectors),
        (sds((16, 15, 16, 128), BF16), sds((T, 2, 4, C), BF16), sds((8, C), F32)),
        cost=cost(1),
    )
    kernel_one = exchange(packed, COL)
    route = [p for x in range(3) for p in ((4 * x + 3, 4 * x + 4), (4 * x + 4, 4 * x + 3))]
    edge = lax.ppermute(edge, COL, route)
    joined = call(join_kernel, (source, edge), sds((T, 6, 4, C), BF16), cost=cost(1))
    wide = lax.all_gather(joined, JAX_, axis=0, tiled=False)
    copies = call(copies_kernel, (weight_two,), sds((4, *weight_two.shape), BF16), cost=cost(1))
    kernel_two = exchange(copies, "x")
    hidden, stats = call(
        conv_one_kernel,
        (wide, kernel_one, vec),
        (sds((4, T, ROW, 128), BF16), sds((8, 128), F32)),
        (pltpu.VMEM((4, T + 2, ROW, C), BF16), pltpu.VMEM((9, C, C), BF16)),
        cost=cost(4),
    )
    stats = lax.psum(stats, "x")
    part = call(
        conv_two_kernel,
        (hidden, stats, kernel_two, vec),
        sds((4, T, 4, 4, C), BF16),
        (pltpu.VMEM((4, T + 2, 16, C), BF16), pltpu.VMEM((9, C, C), BF16)),
        cost=cost(4),
    )
    part = exchange(part, JAX_)
    tail = call(tail_kernel, (part, source, vec), sds((OVMAX, 4, 4, C), BF16), cost=cost(1))
    tiles = lax.axis_size(TILE)
    received = lax.ppermute(tail, TILE, [(i, i + 1) for i in range(tiles - 1)])
    out = pl.pallas_call(
        blend_kernel,
        out_shape=sds((T, 4, 4, C), BF16),
        in_specs=[pl.BlockSpec(memory_space=pltpu.SMEM)] + [whole()] * 5,
        out_specs=whole(),
        compiler_params=PARAMS,
        cost_estimate=cost(1),
    )(intersections, part, tail, source, vec, received)
    return out[None]


def solution(mesh):
    wide = Mesh(mesh.devices.reshape(8, 4, 4, 2, 2), ("z", "yh", "x", "yl", "core"))
    image = P(TILE, None, None, COL, None)
    kernel = P(None, None, None, COL, None)
    in_specs = (image, P(TILE), P(), P(), kernel, P(), P(), kernel, P())
    return jax.shard_map(block, mesh=wide, in_specs=in_specs, out_specs=image, check_vma=False)
```

```python
import jax
import jax.numpy as jnp
from jax import lax
from jax.experimental import pallas as pl
from jax.experimental.pallas import tpu as pltpu
from jax.sharding import Mesh
from jax.sharding import PartitionSpec as P

GROUPS = 32
OVMAX = 4
epsilon = 1e-06
F32, BF16 = jnp.float32, jnp.bfloat16

COL = ("x", "yl", "core")
JAX_ = ("yl", "core")
TILE = ("z", "yh")
T, H, W, C = 17, 4, 64, 256
ROW = 24
PARAMS = pltpu.CompilerParams(vmem_limit_bytes=48 * 1024 * 1024)


def whole():
    return pl.BlockSpec(memory_space=pltpu.VMEM)


def call(kernel, inputs, out_shape, scratch=(), cost=None):
    return pl.pallas_call(
        kernel,
        out_shape=out_shape,
        in_specs=[whole()] * len(inputs),
        out_specs=jax.tree.map(lambda _: whole(), out_shape),
        scratch_shapes=list(scratch),
        compiler_params=PARAMS,
        cost_estimate=cost,
    )(*inputs)


def cost(us):
    return pl.CostEstimate(flops=int(us * 4e8), bytes_accessed=1 << 20, transcendentals=0)


def lanes(shape):
    return lax.broadcasted_iota(jnp.int32, shape, len(shape) - 1)


def rows(shape):
    return lax.broadcasted_iota(jnp.int32, shape, len(shape) - 2)


def split3(value):
    high = value.astype(BF16)
    rest = value - high.astype(F32)
    middle = rest.astype(BF16)
    return high, middle, (rest - middle.astype(F32)).astype(BF16)


def group_sum(value):
    lane, width = lanes(value.shape), value.shape[1]
    for k in (1, 2, 4):
        up, down = pltpu.roll(value, k, 1), pltpu.roll(value, width - k, 1)
        value = value + jnp.where((lane & k) != 0, up, down)
    return value


def group_stats(total, squares):
    members = T * H * W * (C // GROUPS)
    mean = group_sum(total) / members
    spread = jnp.maximum(group_sum(squares) / members - mean * mean, 0.0)
    return mean, lax.rsqrt(spread + epsilon)


def silu(v):
    return v * (0.5 * jnp.tanh(0.5 * v) + 0.5)


def pack_kernel(w_ref, latent_ref, g1_ref, s1_ref, g2_ref, s2_ref, b_ref, n_ref, out_ref, vec_ref):
    for i, ref in enumerate((g1_ref, s1_ref, g2_ref, s2_ref, b_ref)):
        vec_ref[i : i + 1] = ref[...]
    vec_ref[5:6] = jnp.broadcast_to(n_ref[...].astype(F32), (1, C))
    vec_ref[6:8] = jnp.zeros((2, C), F32)
    total, squares = jnp.zeros((4, C), F32), jnp.zeros((4, C), F32)
    for t in range(T):
        for h in range(H):
            v = latent_ref[t, h].astype(F32)
            total += v
            squares += v * v
    pieces = []
    for value in (total, squares):
        for piece in split3(jnp.sum(value, axis=0, keepdims=True)):
            piece = piece.astype(F32)
            pieces += [piece[:, 0:128], piece[:, 128:256]]
    sums = jnp.concatenate(pieces + [jnp.zeros((4, 128), F32)], axis=0).astype(BF16)
    for d in range(16):
        out_ref[d, 14] = sums
    row, col = rows((C, C)), lanes((C, C))
    source = 64 * ((col // 16) % 4) + 16 * (col // 64) + col % 16
    swapped = col ^ 64
    other = 64 * ((swapped // 16) % 4) + 16 * (swapped // 64) + swapped % 16
    left = lanes((16, 128)) < 64
    w = w_ref[...].reshape(27 * 16, C)
    same = jnp.dot(w, (row == source).astype(BF16), preferred_element_type=F32)
    swap = jnp.dot(w, (row == other).astype(BF16), preferred_element_type=F32)

    def block(array, k, dw, j):
        dt, dh = k % 3, k // 3
        at = ((dt * 3 + dh) * 3 + dw) * 16
        return array[at : at + 16, 128 * (j // 2) : 128 * (j // 2) + 128]

    for j in range(4):
        first, second = (same, swap) if j % 2 == 0 else (swap, same)
        for m in range(14):
            if m < 9:
                a, b = block(first, m, 0, j), block(second, m, 1, j)
            else:
                a = block(first, m - 9, 2, j)
                b = block(second, m - 4, 2, j) if m < 13 else jnp.zeros((16, 128), F32)
            tile = jnp.where(left, a, b).astype(BF16)
            for x in range(4):
                out_ref[4 * x + j, m] = tile


def join_kernel(latent_ref, other_ref, near_ref, far_ref, out_ref):
    out_ref[0] = latent_ref[...]
    out_ref[1] = other_ref[...]
    straight = lax.axis_index("yl") == lax.axis_index("core")

    @pl.when(straight)
    def _():
        out_ref[2] = near_ref[...]

    @pl.when(jnp.logical_not(straight))
    def _():
        out_ref[2] = far_ref[...]


def conv_one_kernel(l_ref, w_ref, vec_ref, hid_ref, st_ref, act, wm):
    me = lax.axis_index("x")
    left = lanes((16, 128)) < 64
    nothing = jnp.zeros((16, 128), BF16)
    for p in range(16):
        for k in range(9):
            wm[k, 16 * p : 16 * p + 16, 0:128] = w_ref[p, k]
            if k < 5:
                last = jnp.where(left, w_ref[p, 9 + k], nothing)
            else:
                last = jnp.where(left, nothing, w_ref[p, 4 + k])
            wm[k, 16 * p : 16 * p + 16, 128:256] = last
    sums = sum(w_ref[p, 14].astype(F32) for p in range(16))
    joined = lambda i: jnp.concatenate(
        [sums[i + k : i + k + 1] + sums[i + k + 2 : i + k + 3] + sums[i + k + 4 : i + k + 5] for k in range(2)],
        axis=1,
    )
    total = jnp.broadcast_to(joined(0), (8, C))
    squares = jnp.broadcast_to(joined(6), (8, C))
    mean, inv = group_stats(total, squares)
    scale = inv * vec_ref[0:1]
    mean, scale = mean[0:1], scale[0:1]
    shift = vec_ref[1:2]
    yl = lax.axis_index("yl")
    slots = (yl, 1 - yl)
    row = rows((ROW, C))
    inside = (row >= jnp.where(me == 0, 4, 0)) & (row < jnp.where(me == 3, 20, ROW))
    act[:, 0:2] = jnp.zeros((4, 2, ROW, C), BF16)

    def frame(t, _):
        for h in range(4):
            lo = l_ref[0, 2, t, h].astype(F32)
            hi = l_ref[1, 2, t, h].astype(F32)
            own = [l_ref[q % 2, slots[q // 2], t, h].astype(F32) for q in range(4)]
            v = jnp.concatenate([lo, *own, hi], axis=0)
            y = silu((v - mean) * scale + shift)
            act[h, t + 2] = jnp.where(inside, y, 0.0).astype(BF16)
        return 0

    lax.fori_loop(0, T, frame, 0)

    size = T * ROW
    lane = lanes((size, 128))
    place = rows((size, 128)) % ROW
    own = (place >= 4) & (place < 20)
    s1, s2 = jnp.zeros((1, 128), F32), jnp.zeros((1, 128), F32)
    for h in range(4):
        taps = [dh for dh in range(3) if 0 <= h + dh - 1 < 4]
        lhs = jnp.concatenate(
            [act[h + dh - 1, dt : dt + T].reshape(size, C) for dh in taps for dt in range(3)], axis=1
        )
        rhs = wm[3 * taps[0] : 3 * taps[-1] + 3].reshape(-1, C)
        y = jnp.dot(lhs, rhs, preferred_element_type=F32)
        y0, y1 = y[:, 0:128], y[:, 128:256]
        z = jnp.where(lane < 64, pltpu.roll(y0, 1, 0), y0) + pltpu.roll(y1, size - 1, 0)
        hidden = (z + pltpu.roll(z, 64, 1)).astype(BF16)
        hid_ref[h] = hidden.reshape(T, ROW, 128)
        counted = jnp.where(own, hidden.astype(F32), 0.0)
        s1 += jnp.sum(counted, axis=0, keepdims=True)
        s2 += jnp.sum(counted * counted, axis=0, keepdims=True)
    stats = jnp.concatenate([s1, s2, jnp.zeros((6, 128), F32)], axis=0)
    for d in range(4):
        st_ref[d] = stats


def conv_two_kernel(hid_ref, st_ref, w0_ref, w1_ref, w2_ref, w3_ref, vec_ref, part_ref, act, wm):
    me = lax.axis_index("x")
    j = 2 * lax.axis_index("yl") + lax.axis_index("core")
    for step, w_ref in enumerate((w0_ref, w1_ref, w2_ref, w3_ref)):
        x = lax.rem(me + 4 - step, 4)
        for k in range(9):
            for dw in range(3):
                at = pl.multiple_of(64 * dw + 16 * x, 16)
                wm[k, pl.ds(at, 16)] = w_ref[k % 3, k // 3, dw]
    for k in range(9):
        wm[k, 192:256] = jnp.zeros((64, C), BF16)
    stats = st_ref[0] + st_ref[1] + st_ref[2] + st_ref[3]
    mean, inv = group_stats(
        jnp.broadcast_to(stats[0:1], (8, 128)), jnp.broadcast_to(stats[1:2], (8, 128))
    )
    row, lane = rows((C, 128)), lanes((C, 128))
    mine = (row == 64 * ((lane // 16) % 4) + 16 * j + lane % 16).astype(F32)
    picked = jnp.dot(vec_ref[...], mine, precision=lax.Precision.HIGHEST, preferred_element_type=F32)
    scale, shift = inv[0:1] * picked[2:3], picked[3:4]
    mean = mean[0:1]
    row = rows((ROW, 128))
    inside = (row >= jnp.where(me == 0, 4, 0)) & (row < jnp.where(me == 3, 20, ROW))
    left = lanes((16, 128)) < 64
    act[:, 0:2] = jnp.zeros((4, 2, 16, C), BF16)

    def frame(t, _):
        for h in range(4):
            v = hid_ref[h, t].astype(F32)
            y = silu((v - mean) * scale + shift)
            y = jnp.where(inside, y, 0.0)
            a0, a1, a2 = (pltpu.roll(y, ROW - 3 - dw, 0)[0:16] for dw in range(3))
            act[h, t + 2, :, 0:128] = jnp.where(left, a0, a1).astype(BF16)
            act[h, t + 2, :, 128:256] = jnp.where(left, a2, 0.0).astype(BF16)
        return 0

    lax.fori_loop(0, T, frame, 0)
    for h in range(4):
        taps = [dh for dh in range(3) if 0 <= h + dh - 1 < 4]
        lhs = jnp.concatenate(
            [act[h + dh - 1, dt : dt + T].reshape(T * 16, C) for dh in taps for dt in range(3)], axis=1
        )
        rhs = wm[3 * taps[0] : 3 * taps[-1] + 3].reshape(-1, C)
        y = jnp.dot(lhs, rhs, preferred_element_type=F32).reshape(T, 16, C)
        for d in range(4):
            part_ref[d, :, h] = y[:, 4 * d : 4 * d + 4].astype(BF16)


def decode(part_ref, at, latent, bias):
    branch = part_ref[0, at].astype(F32)
    for q in range(1, 4):
        branch = branch + part_ref[q, at].astype(F32)
    return (latent.astype(F32) + (branch + bias)).astype(BF16)


def tail_kernel(part_ref, latent_ref, vec_ref, tail_ref):
    for i in range(OVMAX):
        tail_ref[i] = decode(part_ref, T - OVMAX + i, latent_ref[T - OVMAX + i], vec_ref[4:5])


def blend_kernel(main_ref, tail_ref, latent_ref, vec_ref, received_ref, out_ref):
    bias, shared = vec_ref[4:5], vec_ref[5:6]
    for t in range(T):
        if t >= T - OVMAX:
            out_ref[t] = tail_ref[t - T + OVMAX]
            continue
        own = decode(main_ref, t, latent_ref[t], bias)
        if t < OVMAX:
            other = received_ref[OVMAX - 1].astype(F32)
            for n in range(t + 2, OVMAX + 1):
                other = jnp.where((shared == n)[None], received_ref[OVMAX - n + t].astype(F32), other)
            share = jnp.full((1, C), t + 1, F32) / (shared + 1.0)
            head = own.astype(F32)
            mixed = share * head + (1.0 - share) * other
            own = jnp.where((shared > t)[None], mixed, head).astype(BF16)
        out_ref[t] = own


def exchange(array, axis):
    return lax.all_to_all(array, axis, split_axis=0, concat_axis=0, tiled=True)


def block(latent, intersections, gain_one, shift_one, weight_one, gain_two, shift_two, weight_two, bias):
    source = latent[0]
    flat = lambda v: v.reshape(1, C)
    sds = jax.ShapeDtypeStruct
    vectors = tuple(flat(v) for v in (gain_one, shift_one, gain_two, shift_two, bias))
    other = lax.ppermute(source, "yl", [(0, 1), (1, 0)])
    near = [p for x in range(3) for p in ((4 * x + 3, 4 * x + 4), (4 * x + 4, 4 * x + 3))]
    far = [p for x in range(3) for p in ((4 * x + 3, 4 * x + 6), (4 * x + 4, 4 * x + 1))]
    near = lax.ppermute(source, COL, near)
    far = lax.ppermute(source, COL, far)
    packed, vec = call(
        pack_kernel,
        (weight_one, source, *vectors, intersections.reshape(1, 1)),
        (sds((16, 15, 16, 128), BF16), sds((8, C), F32)),
        cost=cost(1),
    )
    kernel_one = exchange(packed, COL)
    joined = call(join_kernel, (source, other, near, far), sds((3, T, 4, 4, C), BF16), cost=cost(1))
    wide = lax.all_gather(joined, "core", axis=0, tiled=False)
    kernel_two = [weight_two]
    for step in range(1, 4):
        kernel_two.append(lax.ppermute(weight_two, "x", [(x, (x + step) % 4) for x in range(4)]))
    hidden, stats = call(
        conv_one_kernel,
        (wide, kernel_one, vec),
        (sds((4, T, ROW, 128), BF16), sds((4, 8, 128), F32)),
        (pltpu.VMEM((4, T + 2, ROW, C), BF16), pltpu.VMEM((9, C, C), BF16)),
        cost=cost(4),
    )
    stats = exchange(stats, "x")
    part = call(
        conv_two_kernel,
        (hidden, stats, *kernel_two, vec),
        sds((4, T, 4, 4, C), BF16),
        (pltpu.VMEM((4, T + 2, 16, C), BF16), pltpu.VMEM((9, C, C), BF16)),
        cost=cost(4),
    )
    part = exchange(part, JAX_)
    tail = call(tail_kernel, (part, source, vec), sds((OVMAX, 4, 4, C), BF16), cost=cost(1))
    tiles = lax.axis_size(TILE)
    received = lax.ppermute(tail, TILE, [(i, i + 1) for i in range(tiles - 1)])
    out = call(blend_kernel, (part, tail, source, vec, received), sds((T, 4, 4, C), BF16), cost=cost(1))
    return out[None]


def solution(mesh):
    wide = Mesh(mesh.devices.reshape(8, 4, 4, 2, 2), ("z", "yh", "x", "yl", "core"))
    image = P(TILE, None, None, COL, None)
    kernel = P(None, None, None, COL, None)
    in_specs = (image, P(TILE), P(), P(), kernel, P(), P(), kernel, P())
    return jax.shard_map(block, mesh=wide, in_specs=in_specs, out_specs=image, check_vma=False)
```

```python
import jax
import jax.numpy as jnp
from jax import lax
from jax.experimental import pallas as pl
from jax.experimental.pallas import tpu as pltpu
from jax.sharding import Mesh
from jax.sharding import PartitionSpec as P

GROUPS = 32
OVMAX = 4
epsilon = 1e-06
F32, BF16 = jnp.float32, jnp.bfloat16

COL = ("x", "yl", "core")
JAX_ = ("yl", "core")
TILE = ("z", "yh")
T, H, W, C = 17, 4, 64, 256
ROW = 24
PARAMS = pltpu.CompilerParams(vmem_limit_bytes=48 * 1024 * 1024)


def whole():
    return pl.BlockSpec(memory_space=pltpu.VMEM)


def call(kernel, inputs, out_shape, scratch=(), cost=None):
    return pl.pallas_call(
        kernel,
        out_shape=out_shape,
        in_specs=[whole()] * len(inputs),
        out_specs=jax.tree.map(lambda _: whole(), out_shape),
        scratch_shapes=list(scratch),
        compiler_params=PARAMS,
        cost_estimate=cost,
    )(*inputs)


def cost(us):
    return pl.CostEstimate(flops=int(us * 4e8), bytes_accessed=1 << 20, transcendentals=0)


def lanes(shape):
    return lax.broadcasted_iota(jnp.int32, shape, len(shape) - 1)


def rows(shape):
    return lax.broadcasted_iota(jnp.int32, shape, len(shape) - 2)


def split3(value):
    high = value.astype(BF16)
    rest = value - high.astype(F32)
    middle = rest.astype(BF16)
    return high, middle, (rest - middle.astype(F32)).astype(BF16)


def group_sum(value):
    lane, width = lanes(value.shape), value.shape[1]
    for k in (1, 2, 4):
        up, down = pltpu.roll(value, k, 1), pltpu.roll(value, width - k, 1)
        value = value + jnp.where((lane & k) != 0, up, down)
    return value


def group_stats(total, squares):
    members = T * H * W * (C // GROUPS)
    mean = group_sum(total) / members
    spread = jnp.maximum(group_sum(squares) / members - mean * mean, 0.0)
    return mean, lax.rsqrt(spread + epsilon)


def silu(v):
    return v * (0.5 * jnp.tanh(0.5 * v) + 0.5)


def pack_kernel(
    w_hbm, latent_hbm, g1, s1, g2, s2, b, out_ref, vec_ref, w_ref, latent_ref, line, sems
):
    copies = [
        pltpu.make_async_copy(source, target, sems.at[i])
        for i, (source, target) in enumerate(
            [(latent_hbm, latent_ref), (w_hbm, w_ref)]
            + [(source, line.at[i]) for i, source in enumerate((g1, s1, g2, s2, b))]
        )
    ]
    for copy in copies:
        copy.start()
    for copy in copies:
        copy.wait()
    for i in range(5):
        vec_ref[i : i + 1] = line[i]
    vec_ref[5:8] = jnp.zeros((3, C), F32)
    totals, powers = [], []
    for h in range(H):
        total, squares = jnp.zeros((4, C), F32), jnp.zeros((4, C), F32)
        for t in range(T):
            v = latent_ref[t, h].astype(F32)
            total += v
            squares += v * v
        totals.append(total)
        powers.append(squares)
    total = (totals[0] + totals[1]) + (totals[2] + totals[3])
    squares = (powers[0] + powers[1]) + (powers[2] + powers[3])
    pieces = []
    for value in (total, squares):
        for piece in split3(jnp.sum(value, axis=0, keepdims=True)):
            piece = piece.astype(F32)
            pieces += [piece[:, 0:128], piece[:, 128:256]]
    sums = jnp.concatenate(pieces + [jnp.zeros((4, 128), F32)], axis=0).astype(BF16)
    for d in range(16):
        out_ref[d, 14] = sums
    row, col = rows((C, C)), lanes((C, C))
    source = 64 * ((col // 16) % 4) + 16 * (col // 64) + col % 16
    swapped = col ^ 64
    other = 64 * ((swapped // 16) % 4) + 16 * (swapped // 64) + swapped % 16
    left = lanes((16, 128)) < 64
    w = w_ref[...].reshape(27 * 16, C)
    same = jnp.dot(w, (row == source).astype(BF16), preferred_element_type=F32)
    swap = jnp.dot(w, (row == other).astype(BF16), preferred_element_type=F32)

    def block(array, k, dw, j):
        dt, dh = k % 3, k // 3
        at = ((dt * 3 + dh) * 3 + dw) * 16
        return array[at : at + 16, 128 * (j // 2) : 128 * (j // 2) + 128]

    for j in range(4):
        first, second = (same, swap) if j % 2 == 0 else (swap, same)
        for m in range(14):
            if m < 9:
                a, b = block(first, m, 0, j), block(second, m, 1, j)
            else:
                a = block(first, m - 9, 2, j)
                b = block(second, m - 4, 2, j) if m < 13 else jnp.zeros((16, 128), F32)
            tile = jnp.where(left, a, b).astype(BF16)
            for x in range(4):
                out_ref[4 * x + j, m] = tile


def join_kernel(latent_ref, other_ref, near_ref, far_ref, out_ref):
    out_ref[0] = latent_ref[...]
    out_ref[1] = other_ref[...]
    straight = lax.axis_index("yl") == lax.axis_index("core")

    @pl.when(straight)
    def _():
        out_ref[2] = near_ref[...]

    @pl.when(jnp.logical_not(straight))
    def _():
        out_ref[2] = far_ref[...]


def conv_one_kernel(l_ref, w_ref, vec_ref, hid_ref, st_ref, act, wm):
    me = lax.axis_index("x")
    left = lanes((16, 128)) < 64
    nothing = jnp.zeros((16, 128), BF16)
    for p in range(16):
        for k in range(9):
            wm[k, 16 * p : 16 * p + 16, 0:128] = w_ref[p, k]
            if k < 5:
                last = jnp.where(left, w_ref[p, 9 + k], nothing)
            else:
                last = jnp.where(left, nothing, w_ref[p, 4 + k])
            wm[k, 16 * p : 16 * p + 16, 128:256] = last
    sums = sum(w_ref[p, 14].astype(F32) for p in range(16))
    joined = lambda i: jnp.concatenate(
        [sums[i + k : i + k + 1] + sums[i + k + 2 : i + k + 3] + sums[i + k + 4 : i + k + 5] for k in range(2)],
        axis=1,
    )
    total = jnp.broadcast_to(joined(0), (8, C))
    squares = jnp.broadcast_to(joined(6), (8, C))
    mean, inv = group_stats(total, squares)
    scale = inv * vec_ref[0:1]
    mean, scale = mean[0:1], scale[0:1]
    shift = vec_ref[1:2]
    yl = lax.axis_index("yl")
    slots = (yl, 1 - yl)
    row = rows((ROW, C))
    inside = (row >= jnp.where(me == 0, 4, 0)) & (row < jnp.where(me == 3, 20, ROW))
    act[:, 0:2] = jnp.zeros((4, 2, ROW, C), BF16)

    def frame(t, _):
        for h in range(4):
            lo = l_ref[0, 2, t, h].astype(F32)
            hi = l_ref[1, 2, t, h].astype(F32)
            own = [l_ref[q % 2, slots[q // 2], t, h].astype(F32) for q in range(4)]
            v = jnp.concatenate([lo, *own, hi], axis=0)
            y = silu((v - mean) * scale + shift)
            act[h, t + 2] = jnp.where(inside, y, 0.0).astype(BF16)
        return 0

    lax.fori_loop(0, T, frame, 0)

    size = T * ROW
    lane = lanes((size, 128))
    place = rows((size, 128)) % ROW
    own = (place >= 4) & (place < 20)
    s1, s2 = jnp.zeros((1, 128), F32), jnp.zeros((1, 128), F32)
    for h in range(4):
        taps = [dh for dh in range(3) if 0 <= h + dh - 1 < 4]
        lhs = jnp.concatenate(
            [act[h + dh - 1, dt : dt + T].reshape(size, C) for dh in taps for dt in range(3)], axis=1
        )
        rhs = wm[3 * taps[0] : 3 * taps[-1] + 3].reshape(-1, C)
        y = jnp.dot(lhs, rhs, preferred_element_type=F32)
        y0, y1 = y[:, 0:128], y[:, 128:256]
        z = jnp.where(lane < 64, pltpu.roll(y0, 1, 0), y0) + pltpu.roll(y1, size - 1, 0)
        hidden = (z + pltpu.roll(z, 64, 1)).astype(BF16)
        hid_ref[h] = hidden.reshape(T, ROW, 128)
        counted = jnp.where(own, hidden.astype(F32), 0.0)
        s1 += jnp.sum(counted, axis=0, keepdims=True)
        s2 += jnp.sum(counted * counted, axis=0, keepdims=True)
    stats = jnp.concatenate([s1, s2, jnp.zeros((6, 128), F32)], axis=0)
    for d in range(4):
        st_ref[d] = stats


def conv_two_kernel(hid_ref, st_ref, w0_ref, w1_ref, w2_ref, w3_ref, vec_ref, *outs):
    *parts, act, wm = outs
    tails, mains = parts[:4], parts[4:]
    me = lax.axis_index("x")
    j = 2 * lax.axis_index("yl") + lax.axis_index("core")
    for step, w_ref in enumerate((w0_ref, w1_ref, w2_ref, w3_ref)):
        x = lax.rem(me + 4 - step, 4)
        for k in range(9):
            for dw in range(3):
                at = pl.multiple_of(64 * dw + 16 * x, 16)
                wm[k, pl.ds(at, 16)] = w_ref[k % 3, k // 3, dw]
    for k in range(9):
        wm[k, 192:256] = jnp.zeros((64, C), BF16)
    stats = st_ref[0] + st_ref[1] + st_ref[2] + st_ref[3]
    mean, inv = group_stats(
        jnp.broadcast_to(stats[0:1], (8, 128)), jnp.broadcast_to(stats[1:2], (8, 128))
    )
    row, lane = rows((C, 128)), lanes((C, 128))
    mine = (row == 64 * ((lane // 16) % 4) + 16 * j + lane % 16).astype(F32)
    picked = jnp.dot(vec_ref[...], mine, precision=lax.Precision.HIGHEST, preferred_element_type=F32)
    scale, shift = inv[0:1] * picked[2:3], picked[3:4]
    mean = mean[0:1]
    row = rows((ROW, 128))
    inside = (row >= jnp.where(me == 0, 4, 0)) & (row < jnp.where(me == 3, 20, ROW))
    left = lanes((16, 128)) < 64
    place = jnp.full((8, 128), j, jnp.int32)
    odd, upper = (place & 1) != 0, (place & 2) != 0
    act[:, 0:2] = jnp.zeros((4, 2, 16, C), BF16)

    def frame(t, _):
        for h in range(4):
            v = hid_ref[h, t].astype(F32)
            y = silu((v - mean) * scale + shift)
            y = jnp.where(inside, y, 0.0)
            a0, a1, a2 = (pltpu.roll(y, ROW - 3 - dw, 0)[0:16] for dw in range(3))
            for at, tile in ((0, jnp.where(left, a0, a1)), (128, jnp.where(left, a2, 0.0))):
                low, high = jnp.where(upper, tile[8:16], tile[0:8]), jnp.where(upper, tile[0:8], tile[8:16])
                low = jnp.where(odd, pltpu.roll(low, 4, 0), low)
                high = jnp.where(odd, pltpu.roll(high, 4, 0), high)
                act[h, t + 2, :, at : at + 128] = jnp.concatenate([low, high], axis=0).astype(BF16)
        return 0

    lax.fori_loop(0, T, frame, 0)
    for h in range(4):
        taps = [dh for dh in range(3) if 0 <= h + dh - 1 < 4]
        lhs = jnp.concatenate(
            [act[h + dh - 1, dt : dt + T].reshape(T * 16, C) for dh in taps for dt in range(3)], axis=1
        )
        rhs = wm[3 * taps[0] : 3 * taps[-1] + 3].reshape(-1, C)
        y = jnp.dot(lhs, rhs, preferred_element_type=F32).reshape(T, 16, C)
        for d in range(4):
            columns = y[:, 4 * d : 4 * d + 4].astype(mains[d].dtype)
            mains[d][:, h] = columns[: T - OVMAX]
            tails[d][:, h] = columns[T - OVMAX :]


def decode(parts, at, latent, bias):
    branch = parts[0][at]
    for part in parts[1:]:
        branch = branch + part[at].astype(F32)
    return (latent.astype(F32) + (branch + bias)).astype(BF16)


def tail_kernel(*refs):
    *parts, latent_ref, vec_ref, tail_ref = refs
    for i in range(OVMAX):
        tail_ref[i] = decode(parts, i, latent_ref[T - OVMAX + i], vec_ref[4:5])


def blend_kernel(*refs):
    *parts, tail_ref, latent_ref, vec_ref, shared_ref, received_ref, out_ref = refs
    bias, shared = vec_ref[4:5], shared_ref[...]
    for t in range(T):
        if t >= T - OVMAX:
            out_ref[t] = tail_ref[t - T + OVMAX]
            continue
        own = decode(parts, t, latent_ref[t], bias)
        if t < OVMAX:
            other = received_ref[OVMAX - 1].astype(F32)
            for n in range(t + 2, OVMAX + 1):
                other = jnp.where((shared == n)[None], received_ref[OVMAX - n + t].astype(F32), other)
            share = jnp.full((1, C), t + 1, F32) / (shared + 1.0)
            head = own.astype(F32)
            mixed = share * head + (1.0 - share) * other
            own = jnp.where((shared > t)[None], mixed, head).astype(BF16)
        out_ref[t] = own


def exchange(array, axis):
    return lax.all_to_all(array, axis, split_axis=0, concat_axis=0, tiled=True)


def block(latent, intersections, gain_one, shift_one, weight_one, gain_two, shift_two, weight_two, bias):
    source = latent[0]
    flat = lambda v: v.reshape(1, C)
    sds = jax.ShapeDtypeStruct
    vectors = tuple(flat(v) for v in (gain_one, shift_one, gain_two, shift_two, bias))
    packed, vec = pl.pallas_call(
        pack_kernel,
        out_shape=(sds((16, 15, 16, 128), BF16), sds((8, C), F32)),
        in_specs=[pl.BlockSpec(memory_space=pl.ANY)] * 7,
        out_specs=(whole(), whole()),
        scratch_shapes=[
            pltpu.VMEM(weight_one.shape, BF16),
            pltpu.VMEM(source.shape, BF16),
            pltpu.VMEM((5, 1, C), F32),
            pltpu.SemaphoreType.DMA((7,)),
        ],
        compiler_params=pltpu.CompilerParams(vmem_limit_bytes=67043328),
        cost_estimate=cost(1),
    )(weight_one, source, *vectors)
    kernel_one = exchange(packed, COL)
    other = lax.ppermute(source, "yl", [(0, 1), (1, 0)])
    near = [p for x in range(3) for p in ((4 * x + 3, 4 * x + 4), (4 * x + 4, 4 * x + 3))]
    far = [p for x in range(3) for p in ((4 * x + 3, 4 * x + 6), (4 * x + 4, 4 * x + 1))]
    near = lax.ppermute(source, COL, near)
    far = lax.ppermute(source, COL, far)
    shared = jnp.broadcast_to(intersections.astype(F32).reshape(1, 1), (1, C))
    joined = call(join_kernel, (source, other, near, far), sds((3, T, 4, 4, C), BF16), cost=cost(1))
    wide = lax.all_gather(joined, "core", axis=0, tiled=False)
    kernel_two = [weight_two]
    for step in range(1, 4):
        kernel_two.append(lax.ppermute(weight_two, "x", [(x, (x + step) % 4) for x in range(4)]))
    hidden, stats = call(
        conv_one_kernel,
        (wide, kernel_one, vec),
        (sds((4, T, ROW, 128), BF16), sds((4, 8, 128), F32)),
        (pltpu.VMEM((4, T + 2, ROW, C), BF16), pltpu.VMEM((9, C, C), BF16)),
        cost=cost(4),
    )
    stats = exchange(stats, "x")
    kinds = (F32, BF16, BF16, BF16)
    parts = call(
        conv_two_kernel,
        (hidden, stats, *kernel_two, vec),
        tuple(sds((n, 4, 4, C), kind) for n in (OVMAX, T - OVMAX) for kind in kinds),
        (pltpu.VMEM((4, T + 2, 16, C), BF16), pltpu.VMEM((9, C, C), BF16)),
        cost=cost(4),
    )
    tails, mains = list(parts[:4]), list(parts[4:])
    for arrays in (tails, mains):
        for k in range(1, 4):
            arrays[k] = lax.ppermute(arrays[k], JAX_, [(i, i ^ k) for i in range(4)])
    tail = call(tail_kernel, (*tails, source, vec), sds((OVMAX, 4, 4, C), BF16), cost=cost(1))
    tiles = lax.axis_size(TILE)
    received = lax.ppermute(tail, TILE, [(i, i + 1) for i in range(tiles - 1)])
    out = call(blend_kernel, (*mains, tail, source, vec, shared, received), sds((T, 4, 4, C), BF16), cost=cost(1))
    return out[None]


def solution(mesh):
    wide = Mesh(mesh.devices.reshape(8, 4, 4, 2, 2), ("z", "yh", "x", "yl", "core"))
    image = P(TILE, None, None, COL, None)
    kernel = P(None, None, None, COL, None)
    in_specs = (image, P(TILE), P(), P(), kernel, P(), P(), kernel, P())
    return jax.shard_map(block, mesh=wide, in_specs=in_specs, out_specs=image, check_vma=False)
```

```python
import jax
import jax.numpy as jnp
from jax import lax
from jax.experimental import pallas as pl
from jax.experimental.pallas import tpu as pltpu
from jax.sharding import Mesh
from jax.sharding import PartitionSpec as P

GROUPS = 32
OVMAX = 4
epsilon = 1e-06
F32, BF16 = jnp.float32, jnp.bfloat16

COL = ("x", "yl", "core")
TILE = ("z", "yh")
T, H, W, C = 17, 4, 64, 256
ROW = 24
PARAMS = pltpu.CompilerParams(vmem_limit_bytes=48 * 1024 * 1024)


def whole():
    return pl.BlockSpec(memory_space=pltpu.VMEM)


def call(kernel, inputs, out_shape, scratch=(), cost=None):
    return pl.pallas_call(
        kernel,
        out_shape=out_shape,
        in_specs=[whole()] * len(inputs),
        out_specs=jax.tree.map(lambda _: whole(), out_shape),
        scratch_shapes=list(scratch),
        compiler_params=PARAMS,
        cost_estimate=cost,
    )(*inputs)


def cost(us):
    return pl.CostEstimate(flops=int(us * 4e8), bytes_accessed=1 << 20, transcendentals=0)


def lanes(shape):
    return lax.broadcasted_iota(jnp.int32, shape, len(shape) - 1)


def rows(shape):
    return lax.broadcasted_iota(jnp.int32, shape, len(shape) - 2)


def split3(value):
    high = value.astype(BF16)
    rest = value - high.astype(F32)
    middle = rest.astype(BF16)
    return high, middle, (rest - middle.astype(F32)).astype(BF16)


def group_sum(value):
    lane, width = lanes(value.shape), value.shape[1]
    for k in (1, 2, 4):
        up, down = pltpu.roll(value, k, 1), pltpu.roll(value, width - k, 1)
        value = value + jnp.where((lane & k) != 0, up, down)
    return value


def group_stats(total, squares):
    members = T * H * W * (C // GROUPS)
    mean = group_sum(total) / members
    spread = jnp.maximum(group_sum(squares) / members - mean * mean, 0.0)
    return mean, lax.rsqrt(spread + epsilon)


def silu(v):
    return v * (0.5 * jnp.tanh(0.5 * v) + 0.5)


def pack_kernel(
    w_hbm, latent_hbm, g1, s1, g2, s2, b, out_ref, vec_ref, w_ref, latent_ref, line, sems
):
    copies = [
        pltpu.make_async_copy(source, target, sems.at[i])
        for i, (source, target) in enumerate(
            [(latent_hbm, latent_ref), (w_hbm, w_ref)]
            + [(source, line.at[i]) for i, source in enumerate((g1, s1, g2, s2, b))]
        )
    ]
    for copy in copies:
        copy.start()
    for copy in copies:
        copy.wait()
    for i in range(5):
        vec_ref[i : i + 1] = line[i]
    vec_ref[5:8] = jnp.zeros((3, C), F32)
    totals, powers = [], []
    for h in range(H):
        total, squares = jnp.zeros((4, C), F32), jnp.zeros((4, C), F32)
        for t in range(T):
            v = latent_ref[t, h].astype(F32)
            total += v
            squares += v * v
        totals.append(total)
        powers.append(squares)
    total = (totals[0] + totals[1]) + (totals[2] + totals[3])
    squares = (powers[0] + powers[1]) + (powers[2] + powers[3])
    pieces = []
    for value in (total, squares):
        for piece in split3(jnp.sum(value, axis=0, keepdims=True)):
            piece = piece.astype(F32)
            pieces += [piece[:, 0:128], piece[:, 128:256]]
    sums = jnp.concatenate(pieces + [jnp.zeros((4, 128), F32)], axis=0).astype(BF16)
    for d in range(16):
        out_ref[d, 14] = sums
    row, col = rows((C, C)), lanes((C, C))
    source = 64 * ((col // 16) % 4) + 16 * (col // 64) + col % 16
    swapped = col ^ 64
    other = 64 * ((swapped // 16) % 4) + 16 * (swapped // 64) + swapped % 16
    left = lanes((16, 128)) < 64
    w = w_ref[...].reshape(27 * 16, C)
    same = jnp.dot(w, (row == source).astype(BF16), preferred_element_type=F32)
    swap = jnp.dot(w, (row == other).astype(BF16), preferred_element_type=F32)

    def block(array, k, dw, j):
        dt, dh = k % 3, k // 3
        at = ((dt * 3 + dh) * 3 + dw) * 16
        return array[at : at + 16, 128 * (j // 2) : 128 * (j // 2) + 128]

    for j in range(4):
        first, second = (same, swap) if j % 2 == 0 else (swap, same)
        for m in range(14):
            if m < 9:
                a, b = block(first, m, 0, j), block(second, m, 1, j)
            else:
                a = block(first, m - 9, 2, j)
                b = block(second, m - 4, 2, j) if m < 13 else jnp.zeros((16, 128), F32)
            tile = jnp.where(left, a, b).astype(BF16)
            for x in range(4):
                out_ref[4 * x + j, m] = tile


def join_kernel(n_ref, latent_ref, other_ref, near_ref, far_ref, out_ref, shared_ref):
    shared_ref[...] = jnp.full((1, C), n_ref[0], jnp.int32).astype(F32)
    out_ref[0] = latent_ref[...]
    out_ref[1] = other_ref[...]
    straight = lax.axis_index("yl") == lax.axis_index("core")

    @pl.when(straight)
    def _():
        out_ref[2] = near_ref[...]

    @pl.when(jnp.logical_not(straight))
    def _():
        out_ref[2] = far_ref[...]


def conv_one_kernel(l_ref, w_ref, vec_ref, hid_ref, st_ref, act, wm):
    me = lax.axis_index("x")
    left = lanes((16, 128)) < 64
    nothing = jnp.zeros((16, 128), BF16)
    for p in range(16):
        for k in range(9):
            wm[k, 16 * p : 16 * p + 16, 0:128] = w_ref[p, k]
            if k < 5:
                last = jnp.where(left, w_ref[p, 9 + k], nothing)
            else:
                last = jnp.where(left, nothing, w_ref[p, 4 + k])
            wm[k, 16 * p : 16 * p + 16, 128:256] = last
    sums = sum(w_ref[p, 14].astype(F32) for p in range(16))
    joined = lambda i: jnp.concatenate(
        [sums[i + k : i + k + 1] + sums[i + k + 2 : i + k + 3] + sums[i + k + 4 : i + k + 5] for k in range(2)],
        axis=1,
    )
    total = jnp.broadcast_to(joined(0), (8, C))
    squares = jnp.broadcast_to(joined(6), (8, C))
    mean, inv = group_stats(total, squares)
    scale = inv * vec_ref[0:1]
    mean, scale = mean[0:1], scale[0:1]
    shift = vec_ref[1:2]
    yl = lax.axis_index("yl")
    slots = (yl, 1 - yl)
    row = rows((ROW, C))
    inside = (row >= jnp.where(me == 0, 4, 0)) & (row < jnp.where(me == 3, 20, ROW))
    act[:, 0:2] = jnp.zeros((4, 2, ROW, C), BF16)

    def frame(t, _):
        for h in range(4):
            lo = l_ref[0, 2, t, h].astype(F32)
            hi = l_ref[1, 2, t, h].astype(F32)
            own = [l_ref[q % 2, slots[q // 2], t, h].astype(F32) for q in range(4)]
            v = jnp.concatenate([lo, *own, hi], axis=0)
            y = silu((v - mean) * scale + shift)
            act[h, t + 2] = jnp.where(inside, y, 0.0).astype(BF16)
        return 0

    lax.fori_loop(0, T, frame, 0)

    size = T * ROW
    lane = lanes((size, 128))
    place = rows((size, 128)) % ROW
    own = (place >= 4) & (place < 20)
    s1, s2 = jnp.zeros((1, 128), F32), jnp.zeros((1, 128), F32)
    for h in range(4):
        taps = [dh for dh in range(3) if 0 <= h + dh - 1 < 4]
        lhs = jnp.concatenate(
            [act[h + dh - 1, dt : dt + T].reshape(size, C) for dh in taps for dt in range(3)], axis=1
        )
        rhs = wm[3 * taps[0] : 3 * taps[-1] + 3].reshape(-1, C)
        y = jnp.dot(lhs, rhs, preferred_element_type=F32)
        y0, y1 = y[:, 0:128], y[:, 128:256]
        z = jnp.where(lane < 64, pltpu.roll(y0, 1, 0), y0) + pltpu.roll(y1, size - 1, 0)
        hidden = (z + pltpu.roll(z, 64, 1)).astype(BF16)
        hid_ref[h] = hidden.reshape(T, ROW, 128)
        counted = jnp.where(own, hidden.astype(F32), 0.0)
        s1 += jnp.sum(counted, axis=0, keepdims=True)
        s2 += jnp.sum(counted * counted, axis=0, keepdims=True)
    stats = jnp.concatenate([s1, s2, jnp.zeros((6, 128), F32)], axis=0)
    for d in range(4):
        st_ref[d] = stats


def conv_two_kernel(hid_ref, st_ref, w0_ref, w1_ref, w2_ref, w3_ref, vec_ref, home_ref, away_ref, act, wm):
    me = lax.axis_index("x")
    j = 2 * lax.axis_index("yl") + lax.axis_index("core")
    for step, w_ref in enumerate((w0_ref, w1_ref, w2_ref, w3_ref)):
        x = lax.rem(me + 4 - step, 4)
        for k in range(9):
            for dw in range(3):
                at = pl.multiple_of(64 * dw + 16 * x, 16)
                wm[k, pl.ds(at, 16)] = w_ref[k % 3, k // 3, dw]
    for k in range(9):
        wm[k, 192:256] = jnp.zeros((64, C), BF16)
    stats = st_ref[0] + st_ref[1] + st_ref[2] + st_ref[3]
    mean, inv = group_stats(
        jnp.broadcast_to(stats[0:1], (8, 128)), jnp.broadcast_to(stats[1:2], (8, 128))
    )
    row, lane = rows((C, 128)), lanes((C, 128))
    mine = (row == 64 * ((lane // 16) % 4) + 16 * j + lane % 16).astype(F32)
    picked = jnp.dot(vec_ref[...], mine, precision=lax.Precision.HIGHEST, preferred_element_type=F32)
    scale, shift = inv[0:1] * picked[2:3], picked[3:4]
    mean = mean[0:1]
    row = rows((ROW, 128))
    inside = (row >= jnp.where(me == 0, 4, 0)) & (row < jnp.where(me == 3, 20, ROW))
    left = lanes((16, 128)) < 64
    place = jnp.full((8, 128), j, jnp.int32)
    odd, upper = (place & 1) != 0, (place & 2) != 0
    act[:, 0:2] = jnp.zeros((4, 2, 16, C), BF16)

    def frame(t, _):
        for h in range(4):
            v = hid_ref[h, t].astype(F32)
            y = silu((v - mean) * scale + shift)
            y = jnp.where(inside, y, 0.0)
            a0, a1, a2 = (pltpu.roll(y, ROW - 3 - dw, 0)[0:16] for dw in range(3))
            for at, tile in ((0, jnp.where(left, a0, a1)), (128, jnp.where(left, a2, 0.0))):
                low, high = jnp.where(upper, tile[8:16], tile[0:8]), jnp.where(upper, tile[0:8], tile[8:16])
                low = jnp.where(odd, pltpu.roll(low, 4, 0), low)
                high = jnp.where(odd, pltpu.roll(high, 4, 0), high)
                act[h, t + 2, :, at : at + 128] = jnp.concatenate([low, high], axis=0).astype(BF16)
        return 0

    lax.fori_loop(0, T, frame, 0)
    for h in range(4):
        taps = [dh for dh in range(3) if 0 <= h + dh - 1 < 4]
        lhs = jnp.concatenate(
            [act[h + dh - 1, dt : dt + T].reshape(T * 16, C) for dh in taps for dt in range(3)], axis=1
        )
        rhs = wm[3 * taps[0] : 3 * taps[-1] + 3].reshape(-1, C)
        y = jnp.dot(lhs, rhs, preferred_element_type=F32).reshape(T, 16, C)
        for d in range(4):
            target = away_ref if d % 2 else home_ref
            target[d // 2, :, h] = y[:, 4 * d : 4 * d + 4].astype(target.dtype)


def pair_kernel(home_ref, got_ref, own_ref, tail_ref, main_ref):
    other = 1 - lax.axis_index("core")
    for t in range(T):
        own_ref[t] = home_ref[0, t] + got_ref[other, 0, t].astype(F32)
        send = (home_ref[1, t] + got_ref[other, 1, t].astype(F32)).astype(BF16)
        if t < T - OVMAX:
            main_ref[t] = send
        else:
            tail_ref[t - T + OVMAX] = send


def decode(own, other, latent, bias):
    return (latent.astype(F32) + (own + other.astype(F32) + bias)).astype(BF16)


def tail_kernel(own_ref, other_ref, latent_ref, vec_ref, tail_ref):
    for i in range(OVMAX):
        t = T - OVMAX + i
        tail_ref[i] = decode(own_ref[t], other_ref[i], latent_ref[t], vec_ref[4:5])


def blend_kernel(own_ref, other_ref, tail_ref, latent_ref, vec_ref, shared_ref, received_ref, out_ref):
    bias, shared = vec_ref[4:5], shared_ref[...]
    for t in range(T):
        if t >= T - OVMAX:
            out_ref[t] = tail_ref[t - T + OVMAX]
            continue
        own = decode(own_ref[t], other_ref[t], latent_ref[t], bias)
        if t < OVMAX:
            other = received_ref[OVMAX - 1].astype(F32)
            for n in range(t + 2, OVMAX + 1):
                other = jnp.where((shared == n)[None], received_ref[OVMAX - n + t].astype(F32), other)
            share = jnp.full((1, C), t + 1, F32) / (shared + 1.0)
            head = own.astype(F32)
            mixed = share * head + (1.0 - share) * other
            own = jnp.where((shared > t)[None], mixed, head).astype(BF16)
        out_ref[t] = own


def exchange(array, axis):
    return lax.all_to_all(array, axis, split_axis=0, concat_axis=0, tiled=True)


def block(latent, intersections, gain_one, shift_one, weight_one, gain_two, shift_two, weight_two, bias):
    source = latent[0]
    flat = lambda v: v.reshape(1, C)
    sds = jax.ShapeDtypeStruct
    vectors = tuple(flat(v) for v in (gain_one, shift_one, gain_two, shift_two, bias))
    packed, vec = pl.pallas_call(
        pack_kernel,
        out_shape=(sds((16, 15, 16, 128), BF16), sds((8, C), F32)),
        in_specs=[pl.BlockSpec(memory_space=pl.ANY)] * 7,
        out_specs=(whole(), whole()),
        scratch_shapes=[
            pltpu.VMEM(weight_one.shape, BF16),
            pltpu.VMEM(source.shape, BF16),
            pltpu.VMEM((5, 1, C), F32),
            pltpu.SemaphoreType.DMA((7,)),
        ],
        compiler_params=pltpu.CompilerParams(vmem_limit_bytes=67043328),
        cost_estimate=cost(1),
    )(weight_one, source, *vectors)
    kernel_one = exchange(packed, COL)
    other = lax.ppermute(source, "yl", [(0, 1), (1, 0)])
    near = [p for x in range(3) for p in ((4 * x + 3, 4 * x + 4), (4 * x + 4, 4 * x + 3))]
    far = [p for x in range(3) for p in ((4 * x + 3, 4 * x + 6), (4 * x + 4, 4 * x + 1))]
    near = lax.ppermute(source, COL, near)
    far = lax.ppermute(source, COL, far)
    joined, shared = pl.pallas_call(
        join_kernel,
        out_shape=(sds((3, T, 4, 4, C), BF16), sds((1, C), F32)),
        in_specs=[pl.BlockSpec(memory_space=pltpu.SMEM)] + [whole()] * 4,
        out_specs=(whole(), whole()),
        compiler_params=PARAMS,
        cost_estimate=cost(1),
    )(intersections, source, other, near, far)
    wide = lax.all_gather(joined, "core", axis=0, tiled=False)
    ring = lambda array, step: lax.ppermute(array, "x", [(x, (x + step) % 4) for x in range(4)])
    after = ring(weight_two, 3)
    before = ring(weight_two, 1)
    opposite = ring(after, 3)
    kernel_two = [weight_two, before, opposite, after]
    hidden, stats = call(
        conv_one_kernel,
        (wide, kernel_one, vec),
        (sds((4, T, ROW, 128), BF16), sds((4, 8, 128), F32)),
        (pltpu.VMEM((4, T + 2, ROW, C), BF16), pltpu.VMEM((9, C, C), BF16)),
        cost=cost(4),
    )
    stats, *kernel_two = lax.optimization_barrier((stats, *kernel_two))
    stats = exchange(stats, "x")
    home, away = call(
        conv_two_kernel,
        (hidden, stats, *kernel_two, vec),
        (sds((2, T, 4, 4, C), F32), sds((2, T, 4, 4, C), BF16)),
        (pltpu.VMEM((4, T + 2, 16, C), BF16), pltpu.VMEM((9, C, C), BF16)),
        cost=cost(4),
    )
    got = lax.all_gather(away, "core", axis=0, tiled=False)
    own, rest_tail, rest = call(
        pair_kernel,
        (home, got),
        (sds((T, 4, 4, C), F32), sds((OVMAX, 4, 4, C), BF16), sds((T - OVMAX, 4, 4, C), BF16)),
        cost=cost(1),
    )
    swap = [(0, 1), (1, 0)]
    rest_tail = lax.ppermute(rest_tail, "yl", swap)
    rest = lax.ppermute(rest, "yl", swap)
    tail = call(tail_kernel, (own, rest_tail, source, vec), sds((OVMAX, 4, 4, C), BF16), cost=cost(1))
    tiles = lax.axis_size(TILE)
    received = lax.ppermute(tail, TILE, [(i, i + 1) for i in range(tiles - 1)])
    out = call(blend_kernel, (own, rest, tail, source, vec, shared, received), sds((T, 4, 4, C), BF16), cost=cost(1))
    return out[None]


def solution(mesh):
    wide = Mesh(mesh.devices.reshape(8, 4, 4, 2, 2), ("z", "yh", "x", "yl", "core"))
    image = P(TILE, None, None, COL, None)
    kernel = P(None, None, None, COL, None)
    in_specs = (image, P(TILE), P(), P(), kernel, P(), P(), kernel, P())
    return jax.shard_map(block, mesh=wide, in_specs=in_specs, out_specs=image, check_vma=False)
```

```python
import jax
import jax.numpy as jnp
from jax import lax
from jax.experimental import pallas as pl
from jax.experimental.pallas import tpu as pltpu
from jax.sharding import Mesh
from jax.sharding import PartitionSpec as P

GROUPS = 32
OVMAX = 4
epsilon = 1e-06
F32, BF16 = jnp.float32, jnp.bfloat16

COL = ("x", "yl", "core")
TILE = ("z", "yh")
T, H, W, C = 17, 4, 64, 256
ROW = 24
PARAMS = pltpu.CompilerParams(vmem_limit_bytes=48 * 1024 * 1024)


def whole():
    return pl.BlockSpec(memory_space=pltpu.VMEM)


def call(kernel, inputs, out_shape, scratch=(), cost=None):
    return pl.pallas_call(
        kernel,
        out_shape=out_shape,
        in_specs=[whole()] * len(inputs),
        out_specs=jax.tree.map(lambda _: whole(), out_shape),
        scratch_shapes=list(scratch),
        compiler_params=PARAMS,
        cost_estimate=cost,
    )(*inputs)


def cost(us):
    return pl.CostEstimate(flops=int(us * 4e8), bytes_accessed=1 << 20, transcendentals=0)


def lanes(shape):
    return lax.broadcasted_iota(jnp.int32, shape, len(shape) - 1)


def rows(shape):
    return lax.broadcasted_iota(jnp.int32, shape, len(shape) - 2)


def split3(value):
    high = value.astype(BF16)
    rest = value - high.astype(F32)
    middle = rest.astype(BF16)
    return high, middle, (rest - middle.astype(F32)).astype(BF16)


def group_sum(value):
    lane, width = lanes(value.shape), value.shape[1]
    for k in (1, 2, 4):
        up, down = pltpu.roll(value, k, 1), pltpu.roll(value, width - k, 1)
        value = value + jnp.where((lane & k) != 0, up, down)
    return value


def group_stats(total, squares):
    members = T * H * W * (C // GROUPS)
    mean = group_sum(total) / members
    spread = jnp.maximum(group_sum(squares) / members - mean * mean, 0.0)
    return mean, lax.rsqrt(spread + epsilon)


def silu(v):
    return v * (0.5 * jnp.tanh(0.5 * v) + 0.5)


def pack_kernel(
    w_hbm, latent_hbm, g1, s1, g2, s2, b, out_ref, vec_ref, w_ref, latent_ref, line, sems
):
    copies = [
        pltpu.make_async_copy(source, target, sems.at[i])
        for i, (source, target) in enumerate(
            [(latent_hbm, latent_ref), (w_hbm, w_ref)]
            + [(source, line.at[i]) for i, source in enumerate((g1, s1, g2, s2, b))]
        )
    ]
    for copy in copies:
        copy.start()
    for copy in copies:
        copy.wait()
    for i in range(5):
        vec_ref[i : i + 1] = line[i]
    vec_ref[5:8] = jnp.zeros((3, C), F32)
    totals, powers = [], []
    for h in range(H):
        total, squares = jnp.zeros((4, C), F32), jnp.zeros((4, C), F32)
        for t in range(T):
            v = latent_ref[t, h].astype(F32)
            total += v
            squares += v * v
        totals.append(total)
        powers.append(squares)
    total = (totals[0] + totals[1]) + (totals[2] + totals[3])
    squares = (powers[0] + powers[1]) + (powers[2] + powers[3])
    pieces = []
    for value in (total, squares):
        for piece in split3(jnp.sum(value, axis=0, keepdims=True)):
            piece = piece.astype(F32)
            pieces += [piece[:, 0:128], piece[:, 128:256]]
    sums = jnp.concatenate(pieces + [jnp.zeros((4, 128), F32)], axis=0).astype(BF16)
    for d in range(16):
        out_ref[d, 14] = sums
    row, col = rows((C, C)), lanes((C, C))
    source = 64 * ((col // 16) % 4) + 16 * (col // 64) + col % 16
    swapped = col ^ 64
    other = 64 * ((swapped // 16) % 4) + 16 * (swapped // 64) + swapped % 16
    left = lanes((16, 128)) < 64
    w = w_ref[...].reshape(27 * 16, C)
    same = jnp.dot(w, (row == source).astype(BF16), preferred_element_type=F32)
    swap = jnp.dot(w, (row == other).astype(BF16), preferred_element_type=F32)

    def block(array, k, dw, j):
        dt, dh = k % 3, k // 3
        at = ((dt * 3 + dh) * 3 + dw) * 16
        return array[at : at + 16, 128 * (j // 2) : 128 * (j // 2) + 128]

    for j in range(4):
        first, second = (same, swap) if j % 2 == 0 else (swap, same)
        for m in range(14):
            if m < 9:
                a, b = block(first, m, 0, j), block(second, m, 1, j)
            else:
                a = block(first, m - 9, 2, j)
                b = block(second, m - 4, 2, j) if m < 13 else jnp.zeros((16, 128), F32)
            tile = jnp.where(left, a, b).astype(BF16)
            for x in range(4):
                out_ref[4 * x + j, m] = tile


def join_kernel(n_ref, latent_ref, other_ref, near_ref, far_ref, out_ref, shared_ref):
    shared_ref[...] = jnp.full((1, C), n_ref[0], jnp.int32).astype(F32)
    out_ref[0] = latent_ref[...]
    out_ref[1] = other_ref[...]
    straight = lax.axis_index("yl") == lax.axis_index("core")

    @pl.when(straight)
    def _():
        out_ref[2] = near_ref[...]

    @pl.when(jnp.logical_not(straight))
    def _():
        out_ref[2] = far_ref[...]


def conv_one_kernel(l_ref, w_ref, vec_ref, hid_ref, st_ref, act, wm):
    me = lax.axis_index("x")
    left = lanes((16, 128)) < 64
    nothing = jnp.zeros((16, 128), BF16)
    for p in range(16):
        for k in range(9):
            wm[k, 16 * p : 16 * p + 16, 0:128] = w_ref[p, k]
            if k < 5:
                last = jnp.where(left, w_ref[p, 9 + k], nothing)
            else:
                last = jnp.where(left, nothing, w_ref[p, 4 + k])
            wm[k, 16 * p : 16 * p + 16, 128:256] = last
    sums = sum(w_ref[p, 14].astype(F32) for p in range(16))
    joined = lambda i: jnp.concatenate(
        [sums[i + k : i + k + 1] + sums[i + k + 2 : i + k + 3] + sums[i + k + 4 : i + k + 5] for k in range(2)],
        axis=1,
    )
    total = jnp.broadcast_to(joined(0), (8, C))
    squares = jnp.broadcast_to(joined(6), (8, C))
    mean, inv = group_stats(total, squares)
    scale = inv * vec_ref[0:1]
    mean, scale = mean[0:1], scale[0:1]
    shift = vec_ref[1:2]
    yl = lax.axis_index("yl")
    slots = (yl, 1 - yl)
    row = rows((ROW, C))
    inside = (row >= jnp.where(me == 0, 4, 0)) & (row < jnp.where(me == 3, 20, ROW))
    act[:, 0:2] = jnp.zeros((4, 2, ROW, C), BF16)

    def frame(t, _):
        for h in range(4):
            lo = l_ref[0, 2, t, h].astype(F32)
            hi = l_ref[1, 2, t, h].astype(F32)
            own = [l_ref[q % 2, slots[q // 2], t, h].astype(F32) for q in range(4)]
            v = jnp.concatenate([lo, *own, hi], axis=0)
            y = silu((v - mean) * scale + shift)
            act[h, t + 2] = jnp.where(inside, y, 0.0).astype(BF16)
        return 0

    lax.fori_loop(0, T, frame, 0)

    size = T * ROW
    lane = lanes((size, 128))
    place = rows((size, 128)) % ROW
    own = (place >= 4) & (place < 20)
    s1, s2 = jnp.zeros((1, 128), F32), jnp.zeros((1, 128), F32)
    for h in range(4):
        taps = [dh for dh in range(3) if 0 <= h + dh - 1 < 4]
        lhs = jnp.concatenate(
            [act[h + dh - 1, dt : dt + T].reshape(size, C) for dh in taps for dt in range(3)], axis=1
        )
        rhs = wm[3 * taps[0] : 3 * taps[-1] + 3].reshape(-1, C)
        y = jnp.dot(lhs, rhs, preferred_element_type=F32)
        y0, y1 = y[:, 0:128], y[:, 128:256]
        z = jnp.where(lane < 64, pltpu.roll(y0, 1, 0), y0) + pltpu.roll(y1, size - 1, 0)
        hidden = (z + pltpu.roll(z, 64, 1)).astype(BF16)
        hid_ref[h] = hidden.reshape(T, ROW, 128)
        counted = jnp.where(own, hidden.astype(F32), 0.0)
        s1 += jnp.sum(counted, axis=0, keepdims=True)
        s2 += jnp.sum(counted * counted, axis=0, keepdims=True)
    stats = jnp.concatenate([s1, s2, jnp.zeros((6, 128), F32)], axis=0)
    for d in range(4):
        st_ref[d] = stats


def conv_two_kernel(hid_ref, st_ref, w0_ref, w1_ref, w2_ref, w3_ref, vec_ref, home_ref, away_ref, act, wm):
    me = lax.axis_index("x")
    j = 2 * lax.axis_index("yl") + lax.axis_index("core")
    for step, w_ref in enumerate((w0_ref, w1_ref, w2_ref, w3_ref)):
        x = lax.rem(me + 4 - step, 4)
        for k in range(9):
            for dw in range(3):
                at = pl.multiple_of(64 * dw + 16 * x, 16)
                wm[k, pl.ds(at, 16)] = w_ref[k % 3, k // 3, dw]
    for k in range(9):
        wm[k, 192:256] = jnp.zeros((64, C), BF16)
    stats = st_ref[0] + st_ref[1] + st_ref[2] + st_ref[3]
    mean, inv = group_stats(
        jnp.broadcast_to(stats[0:1], (8, 128)), jnp.broadcast_to(stats[1:2], (8, 128))
    )
    row, lane = rows((C, 128)), lanes((C, 128))
    mine = (row == 64 * ((lane // 16) % 4) + 16 * j + lane % 16).astype(F32)
    picked = jnp.dot(vec_ref[...], mine, precision=lax.Precision.HIGHEST, preferred_element_type=F32)
    scale, shift = inv[0:1] * picked[2:3], picked[3:4]
    mean = mean[0:1]
    row = rows((ROW, 128))
    inside = (row >= jnp.where(me == 0, 4, 0)) & (row < jnp.where(me == 3, 20, ROW))
    left = lanes((16, 128)) < 64
    place = jnp.full((8, 128), j, jnp.int32)
    odd, upper = (place & 1) != 0, (place & 2) != 0
    act[:, 0:2] = jnp.zeros((4, 2, 16, C), BF16)

    def frame(t, _):
        for h in range(4):
            v = hid_ref[h, t].astype(F32)
            y = silu((v - mean) * scale + shift)
            y = jnp.where(inside, y, 0.0)
            a0, a1, a2 = (pltpu.roll(y, ROW - 3 - dw, 0)[0:16] for dw in range(3))
            for at, tile in ((0, jnp.where(left, a0, a1)), (128, jnp.where(left, a2, 0.0))):
                low, high = jnp.where(upper, tile[8:16], tile[0:8]), jnp.where(upper, tile[0:8], tile[8:16])
                low = jnp.where(odd, pltpu.roll(low, 4, 0), low)
                high = jnp.where(odd, pltpu.roll(high, 4, 0), high)
                act[h, t + 2, :, at : at + 128] = jnp.concatenate([low, high], axis=0).astype(BF16)
        return 0

    lax.fori_loop(0, T, frame, 0)
    for h in range(4):
        taps = [dh for dh in range(3) if 0 <= h + dh - 1 < 4]
        lhs = jnp.concatenate(
            [act[h + dh - 1, dt : dt + T].reshape(T * 16, C) for dh in taps for dt in range(3)], axis=1
        )
        rhs = wm[3 * taps[0] : 3 * taps[-1] + 3].reshape(-1, C)
        y = jnp.dot(lhs, rhs, preferred_element_type=F32).reshape(T, 16, C)
        for d in range(4):
            target = away_ref if d % 2 else home_ref
            target[d // 2, :, h] = y[:, 4 * d : 4 * d + 4].astype(target.dtype)


def pair_kernel(home_ref, got_ref, own_ref, tail_ref, main_ref):
    other = 1 - lax.axis_index("core")
    for t in range(T):
        own_ref[t] = home_ref[0, t] + got_ref[other, 0, t].astype(F32)
        send = (home_ref[1, t] + got_ref[other, 1, t].astype(F32)).astype(BF16)
        if t < T - OVMAX:
            main_ref[t] = send
        else:
            tail_ref[t - T + OVMAX] = send


def decode(own, other, latent, bias):
    return (latent.astype(F32) + (own + other.astype(F32) + bias)).astype(BF16)


def tail_kernel(own_ref, other_ref, latent_ref, vec_ref, tail_ref):
    for i in range(OVMAX):
        t = T - OVMAX + i
        tail_ref[i] = decode(own_ref[t], other_ref[i], latent_ref[t], vec_ref[4:5])


def blend_kernel(own_ref, other_ref, tail_ref, latent_ref, vec_ref, shared_ref, received_ref, out_ref):
    bias, shared = vec_ref[4:5], shared_ref[...]
    for t in range(T):
        if t >= T - OVMAX:
            out_ref[t] = tail_ref[t - T + OVMAX]
            continue
        own = decode(own_ref[t], other_ref[t], latent_ref[t], bias)
        if t < OVMAX:
            other = received_ref[OVMAX - 1].astype(F32)
            for n in range(t + 2, OVMAX + 1):
                other = jnp.where((shared == n)[None], received_ref[OVMAX - n + t].astype(F32), other)
            share = jnp.full((1, C), t + 1, F32) / (shared + 1.0)
            head = own.astype(F32)
            mixed = share * head + (1.0 - share) * other
            own = jnp.where((shared > t)[None], mixed, head).astype(BF16)
        out_ref[t] = own


def exchange(array, axis):
    return lax.all_to_all(array, axis, split_axis=0, concat_axis=0, tiled=True)


def block(latent, intersections, gain_one, shift_one, weight_one, gain_two, shift_two, weight_two, bias):
    source = latent[0]
    flat = lambda v: v.reshape(1, C)
    sds = jax.ShapeDtypeStruct
    vectors = tuple(flat(v) for v in (gain_one, shift_one, gain_two, shift_two, bias))
    packed, vec = pl.pallas_call(
        pack_kernel,
        out_shape=(sds((16, 15, 16, 128), BF16), sds((8, C), F32)),
        in_specs=[pl.BlockSpec(memory_space=pl.ANY)] * 7,
        out_specs=(whole(), whole()),
        scratch_shapes=[
            pltpu.VMEM(weight_one.shape, BF16),
            pltpu.VMEM(source.shape, BF16),
            pltpu.VMEM((5, 1, C), F32),
            pltpu.SemaphoreType.DMA((7,)),
        ],
        compiler_params=pltpu.CompilerParams(vmem_limit_bytes=67043328),
        cost_estimate=cost(1),
    )(weight_one, source, *vectors)
    kernel_one = exchange(packed, COL)
    kernel_two = [weight_two]
    for step in range(1, 4):
        kernel_two.append(lax.ppermute(weight_two, "x", [(x, (x + step) % 4) for x in range(4)]))
    other = lax.ppermute(source, "yl", [(0, 1), (1, 0)])
    near = [p for x in range(3) for p in ((4 * x + 3, 4 * x + 4), (4 * x + 4, 4 * x + 3))]
    far = [p for x in range(3) for p in ((4 * x + 3, 4 * x + 6), (4 * x + 4, 4 * x + 1))]
    near = lax.ppermute(source, COL, near)
    far = lax.ppermute(source, COL, far)
    joined, shared = pl.pallas_call(
        join_kernel,
        out_shape=(sds((3, T, 4, 4, C), BF16), sds((1, C), F32)),
        in_specs=[pl.BlockSpec(memory_space=pltpu.SMEM)] + [whole()] * 4,
        out_specs=(whole(), whole()),
        compiler_params=PARAMS,
        cost_estimate=cost(1),
    )(intersections, source, other, near, far)
    wide = lax.all_gather(joined, "core", axis=0, tiled=False)
    hidden, stats = call(
        conv_one_kernel,
        (wide, kernel_one, vec),
        (sds((4, T, ROW, 128), BF16), sds((4, 8, 128), F32)),
        (pltpu.VMEM((4, T + 2, ROW, C), BF16), pltpu.VMEM((9, C, C), BF16)),
        cost=cost(4),
    )
    stats, *kernel_two = lax.optimization_barrier((stats, *kernel_two))
    stats = exchange(stats, "x")
    home, away = call(
        conv_two_kernel,
        (hidden, stats, *kernel_two, vec),
        (sds((2, T, 4, 4, C), F32), sds((2, T, 4, 4, C), BF16)),
        (pltpu.VMEM((4, T + 2, 16, C), BF16), pltpu.VMEM((9, C, C), BF16)),
        cost=cost(4),
    )
    got = lax.all_gather(away, "core", axis=0, tiled=False)
    own, rest_tail, rest = call(
        pair_kernel,
        (home, got),
        (sds((T, 4, 4, C), F32), sds((OVMAX, 4, 4, C), BF16), sds((T - OVMAX, 4, 4, C), BF16)),
        cost=cost(1),
    )
    swap = [(0, 1), (1, 0)]
    rest_tail = lax.ppermute(rest_tail, "yl", swap)
    rest = lax.ppermute(rest, "yl", swap)
    tail = call(tail_kernel, (own, rest_tail, source, vec), sds((OVMAX, 4, 4, C), BF16), cost=cost(1))
    tiles = lax.axis_size(TILE)
    received = lax.ppermute(tail, TILE, [(i, i + 1) for i in range(tiles - 1)])
    out = call(blend_kernel, (own, rest, tail, source, vec, shared, received), sds((T, 4, 4, C), BF16), cost=cost(1))
    return out[None]


def solution(mesh):
    wide = Mesh(mesh.devices.reshape(8, 4, 4, 2, 2), ("z", "yh", "x", "yl", "core"))
    image = P(TILE, None, None, COL, None)
    kernel = P(None, None, None, COL, None)
    in_specs = (image, P(TILE), P(), P(), kernel, P(), P(), kernel, P())
    return jax.shard_map(block, mesh=wide, in_specs=in_specs, out_specs=image, check_vma=False)
```

```python
import jax
import jax.numpy as jnp
from jax import lax
from jax.experimental import pallas as pl
from jax.experimental.pallas import tpu as pltpu
from jax.sharding import Mesh
from jax.sharding import PartitionSpec as P

GROUPS = 32
OVMAX = 4
epsilon = 1e-06
F32, BF16 = jnp.float32, jnp.bfloat16

COL = ("x", "yl", "core")
TILE = ("z", "yh")
T, H, W, C = 17, 4, 64, 256
ROW = 24
PARAMS = pltpu.CompilerParams(vmem_limit_bytes=48 * 1024 * 1024)


def whole():
    return pl.BlockSpec(memory_space=pltpu.VMEM)


def call(kernel, inputs, out_shape, scratch=(), cost=None):
    return pl.pallas_call(
        kernel,
        out_shape=out_shape,
        in_specs=[whole()] * len(inputs),
        out_specs=jax.tree.map(lambda _: whole(), out_shape),
        scratch_shapes=list(scratch),
        compiler_params=PARAMS,
        cost_estimate=cost,
    )(*inputs)


def cost(us):
    return pl.CostEstimate(flops=int(us * 4e8), bytes_accessed=1 << 20, transcendentals=0)


def lanes(shape):
    return lax.broadcasted_iota(jnp.int32, shape, len(shape) - 1)


def rows(shape):
    return lax.broadcasted_iota(jnp.int32, shape, len(shape) - 2)


def split3(value):
    high = value.astype(BF16)
    rest = value - high.astype(F32)
    middle = rest.astype(BF16)
    return high, middle, (rest - middle.astype(F32)).astype(BF16)


def group_sum(value):
    lane, width = lanes(value.shape), value.shape[1]
    for k in (1, 2, 4):
        up, down = pltpu.roll(value, k, 1), pltpu.roll(value, width - k, 1)
        value = value + jnp.where((lane & k) != 0, up, down)
    return value


def moments(total, squares):
    members = T * H * W * (C // GROUPS)
    mean = total / members
    spread = jnp.maximum(squares / members - mean * mean, 0.0)
    return mean, lax.rsqrt(spread + epsilon)


def silu(v):
    return v * (0.5 * jnp.tanh(0.5 * v) + 0.5)


def pack_kernel(
    w_hbm, latent_hbm, g1, s1, g2, s2, b, out_ref, vec_ref, w_ref, latent_ref, line, sems
):
    copies = [
        pltpu.make_async_copy(source, target, sems.at[i])
        for i, (source, target) in enumerate(
            [(latent_hbm, latent_ref), (w_hbm, w_ref)]
            + [(source, line.at[i]) for i, source in enumerate((g1, s1, g2, s2, b))]
        )
    ]
    for copy in copies:
        copy.start()
    for copy in copies:
        copy.wait()
    for i in range(5):
        vec_ref[i : i + 1] = line[i]
    vec_ref[5:8] = jnp.zeros((3, C), F32)
    totals, powers = [], []
    for h in range(H):
        total, squares = jnp.zeros((4, C), F32), jnp.zeros((4, C), F32)
        for t in range(T):
            v = latent_ref[t, h].astype(F32)
            total += v
            squares += v * v
        totals.append(total)
        powers.append(squares)
    total = (totals[0] + totals[1]) + (totals[2] + totals[3])
    squares = (powers[0] + powers[1]) + (powers[2] + powers[3])
    line_sum = jnp.broadcast_to(jnp.sum(total, axis=0, keepdims=True), (8, C))
    line_square = jnp.broadcast_to(jnp.sum(squares, axis=0, keepdims=True), (8, C))
    spot = lanes((8, C)) & 7
    sums = jnp.zeros((8, C), F32)
    for start, value in ((0, group_sum(line_sum)), (3, group_sum(line_square))):
        for i, piece in enumerate(split3(value)):
            sums = jnp.where(spot == start + i, piece.astype(F32), sums)
    halves = [sums[0:1, 0:128], sums[0:1, 128:256]]
    extra = jnp.concatenate(
        [pltpu.roll(sums[:, 0:128], 64, 1)[0:1], halves[0], pltpu.roll(sums[:, 128:256], 64, 1)[0:1], halves[1],
         jnp.zeros((12, 128), F32)],
        axis=0,
    )
    row, col = rows((C, C)), lanes((C, C))
    source = 64 * ((col // 16) % 4) + 16 * (col // 64) + col % 16
    swapped = col ^ 64
    other = 64 * ((swapped // 16) % 4) + 16 * (swapped // 64) + swapped % 16
    left = lanes((16, 128)) < 64
    w = w_ref[...].reshape(27 * 16, C)
    same = jnp.dot(w, (row == source).astype(BF16), preferred_element_type=F32)
    swap = jnp.dot(w, (row == other).astype(BF16), preferred_element_type=F32)

    def block(array, k, dw, j):
        dt, dh = k % 3, k // 3
        at = ((dt * 3 + dh) * 3 + dw) * 16
        return array[at : at + 16, 128 * (j // 2) : 128 * (j // 2) + 128]

    for j in range(4):
        first, second = (same, swap) if j % 2 == 0 else (swap, same)
        for m in range(14):
            if m < 9:
                a, b = block(first, m, 0, j), block(second, m, 1, j)
            else:
                a = block(first, m - 9, 2, j)
                b = block(second, m - 4, 2, j) if m < 13 else extra
            tile = jnp.where(left, a, b).astype(BF16)
            for x in range(4):
                out_ref[4 * x + j, m] = tile


def count_kernel(n_ref, out_ref):
    out_ref[...] = jnp.full((1, C), n_ref[0], jnp.int32).astype(F32)


def join_kernel(latent_ref, other_ref, near_ref, far_ref, out_ref):
    out_ref[0] = latent_ref[...]
    out_ref[1] = other_ref[...]
    straight = lax.axis_index("yl") == lax.axis_index("core")

    @pl.when(straight)
    def _():
        out_ref[2] = near_ref[...]

    @pl.when(jnp.logical_not(straight))
    def _():
        out_ref[2] = far_ref[...]


def conv_one_kernel(l_ref, w_ref, vec_ref, hid_ref, st_ref, act, wm):
    me = lax.axis_index("x")
    left = lanes((16, 128)) < 64
    nothing = jnp.zeros((16, 128), BF16)
    for p in range(16):
        for k in range(9):
            wm[k, 16 * p : 16 * p + 16, 0:128] = w_ref[p, k]
            if k < 5:
                last = jnp.where(left, w_ref[p, 9 + k], nothing)
            else:
                last = jnp.where(left, nothing, w_ref[p, 4 + k])
            wm[k, 16 * p : 16 * p + 16, 128:256] = last
    sums = sum(w_ref[p, 13].astype(F32) for p in range(16))[0:8]
    turned = pltpu.roll(sums, 64, 1)
    first = lanes((1, 128)) < 64
    line = jnp.concatenate(
        [jnp.where(first, turned[2 * i : 2 * i + 1], sums[2 * i + 1 : 2 * i + 2]) for i in range(2)], axis=1
    )
    line = jnp.broadcast_to(line, (8, C))
    spot = lanes((8, C)) & 7
    mean, inv = moments(
        group_sum(jnp.where(spot < 3, line, 0.0)), group_sum(jnp.where((spot > 2) & (spot < 6), line, 0.0))
    )
    scale = inv * vec_ref[0:1]
    mean, scale = mean[0:1], scale[0:1]
    shift = vec_ref[1:2]
    yl = lax.axis_index("yl")
    slots = (yl, 1 - yl)
    row = rows((ROW, C))
    inside = (row >= jnp.where(me == 0, 4, 0)) & (row < jnp.where(me == 3, 20, ROW))
    act[:, 0:2] = jnp.zeros((4, 2, ROW, C), BF16)

    def frame(t, _):
        for h in range(4):
            lo = l_ref[0, 2, t, h].astype(F32)
            hi = l_ref[1, 2, t, h].astype(F32)
            own = [l_ref[q % 2, slots[q // 2], t, h].astype(F32) for q in range(4)]
            v = jnp.concatenate([lo, *own, hi], axis=0)
            y = silu((v - mean) * scale + shift)
            act[h, t + 2] = jnp.where(inside, y, 0.0).astype(BF16)
        return 0

    lax.fori_loop(0, T, frame, 0)

    size = T * ROW
    lane = lanes((size, 128))
    place = rows((size, 128)) % ROW
    own = (place >= 4) & (place < 20)
    s1, s2 = jnp.zeros((1, 128), F32), jnp.zeros((1, 128), F32)
    for h in range(4):
        taps = [dh for dh in range(3) if 0 <= h + dh - 1 < 4]
        lhs = jnp.concatenate(
            [act[h + dh - 1, dt : dt + T].reshape(size, C) for dh in taps for dt in range(3)], axis=1
        )
        rhs = wm[3 * taps[0] : 3 * taps[-1] + 3].reshape(-1, C)
        y = jnp.dot(lhs, rhs, preferred_element_type=F32)
        y0, y1 = y[:, 0:128], y[:, 128:256]
        z = jnp.where(lane < 64, pltpu.roll(y0, 1, 0), y0) + pltpu.roll(y1, size - 1, 0)
        hidden = (z + pltpu.roll(z, 64, 1)).astype(BF16)
        hid_ref[h] = hidden.reshape(T, ROW, 128)
        counted = jnp.where(own, hidden.astype(F32), 0.0)
        s1 += jnp.sum(counted, axis=0, keepdims=True)
        s2 += jnp.sum(counted * counted, axis=0, keepdims=True)
    stats = jnp.concatenate([s1, s2, jnp.zeros((6, 128), F32)], axis=0)
    for d in range(4):
        st_ref[d] = stats


def conv_two_kernel(hid_ref, st_ref, w0_ref, w1_ref, w2_ref, w3_ref, vec_ref, home_ref, away_ref, act, wm):
    me = lax.axis_index("x")
    j = 2 * lax.axis_index("yl") + lax.axis_index("core")
    for step, w_ref in enumerate((w0_ref, w1_ref, w2_ref, w3_ref)):
        x = lax.rem(me + 4 - step, 4)
        for k in range(9):
            for dw in range(3):
                at = pl.multiple_of(64 * dw + 16 * x, 16)
                wm[k, pl.ds(at, 16)] = w_ref[k % 3, k // 3, dw]
    for k in range(9):
        wm[k, 192:256] = jnp.zeros((64, C), BF16)
    stats = st_ref[0] + st_ref[1] + st_ref[2] + st_ref[3]
    mean, inv = moments(
        group_sum(jnp.broadcast_to(stats[0:1], (8, 128))), group_sum(jnp.broadcast_to(stats[1:2], (8, 128)))
    )
    row, lane = rows((C, 128)), lanes((C, 128))
    mine = (row == 64 * ((lane // 16) % 4) + 16 * j + lane % 16).astype(F32)
    picked = jnp.dot(vec_ref[...], mine, precision=lax.Precision.HIGHEST, preferred_element_type=F32)
    scale, shift = inv[0:1] * picked[2:3], picked[3:4]
    mean = mean[0:1]
    row = rows((ROW, 128))
    inside = (row >= jnp.where(me == 0, 4, 0)) & (row < jnp.where(me == 3, 20, ROW))
    left = lanes((16, 128)) < 64
    place = jnp.full((8, 128), j, jnp.int32)
    odd, upper = (place & 1) != 0, (place & 2) != 0
    act[:, 0:2] = jnp.zeros((4, 2, 16, C), BF16)

    def frame(t, _):
        for h in range(4):
            v = hid_ref[h, t].astype(F32)
            y = silu((v - mean) * scale + shift)
            y = jnp.where(inside, y, 0.0)
            a0, a1, a2 = (pltpu.roll(y, ROW - 3 - dw, 0)[0:16] for dw in range(3))
            for at, tile in ((0, jnp.where(left, a0, a1)), (128, jnp.where(left, a2, 0.0))):
                low, high = jnp.where(upper, tile[8:16], tile[0:8]), jnp.where(upper, tile[0:8], tile[8:16])
                low = jnp.where(odd, pltpu.roll(low, 4, 0), low)
                high = jnp.where(odd, pltpu.roll(high, 4, 0), high)
                act[h, t + 2, :, at : at + 128] = jnp.concatenate([low, high], axis=0).astype(BF16)
        return 0

    lax.fori_loop(0, T, frame, 0)
    for h in range(4):
        taps = [dh for dh in range(3) if 0 <= h + dh - 1 < 4]
        lhs = jnp.concatenate(
            [act[h + dh - 1, dt : dt + T].reshape(T * 16, C) for dh in taps for dt in range(3)], axis=1
        )
        rhs = wm[3 * taps[0] : 3 * taps[-1] + 3].reshape(-1, C)
        y = jnp.dot(lhs, rhs, preferred_element_type=F32).reshape(T, 16, C)
        for d in range(4):
            target = away_ref if d % 2 else home_ref
            target[d // 2, :, h] = y[:, 4 * d : 4 * d + 4].astype(target.dtype)


def pair_kernel(home_ref, got_ref, own_ref, tail_ref, main_ref):
    other = 1 - lax.axis_index("core")
    for t in range(T):
        own_ref[t] = home_ref[0, t] + got_ref[other, 0, t].astype(F32)
        send = (home_ref[1, t] + got_ref[other, 1, t].astype(F32)).astype(BF16)
        if t < T - OVMAX:
            main_ref[t] = send
        else:
            tail_ref[t - T + OVMAX] = send


def decode(own, other, latent, bias):
    return (latent.astype(F32) + (own + other.astype(F32) + bias)).astype(BF16)


def tail_kernel(own_ref, other_ref, latent_ref, vec_ref, tail_ref):
    for i in range(OVMAX):
        t = T - OVMAX + i
        tail_ref[i] = decode(own_ref[t], other_ref[i], latent_ref[t], vec_ref[4:5])


def blend_kernel(own_ref, other_ref, tail_ref, latent_ref, vec_ref, shared_ref, received_ref, out_ref):
    bias, shared = vec_ref[4:5], shared_ref[...]
    for t in range(T):
        if t >= T - OVMAX:
            out_ref[t] = tail_ref[t - T + OVMAX]
            continue
        own = decode(own_ref[t], other_ref[t], latent_ref[t], bias)
        if t < OVMAX:
            other = received_ref[OVMAX - 1].astype(F32)
            for n in range(t + 2, OVMAX + 1):
                other = jnp.where((shared == n)[None], received_ref[OVMAX - n + t].astype(F32), other)
            share = jnp.full((1, C), t + 1, F32) / (shared + 1.0)
            head = own.astype(F32)
            mixed = share * head + (1.0 - share) * other
            own = jnp.where((shared > t)[None], mixed, head).astype(BF16)
        out_ref[t] = own


def exchange(array, axis):
    return lax.all_to_all(array, axis, split_axis=0, concat_axis=0, tiled=True)


def block(latent, intersections, gain_one, shift_one, weight_one, gain_two, shift_two, weight_two, bias):
    source = latent[0]
    flat = lambda v: v.reshape(1, C)
    sds = jax.ShapeDtypeStruct
    vectors = tuple(flat(v) for v in (gain_one, shift_one, gain_two, shift_two, bias))
    packed, vec = pl.pallas_call(
        pack_kernel,
        out_shape=(sds((16, 14, 16, 128), BF16), sds((8, C), F32)),
        in_specs=[pl.BlockSpec(memory_space=pl.ANY)] * 7,
        out_specs=(whole(), whole()),
        scratch_shapes=[
            pltpu.VMEM(weight_one.shape, BF16),
            pltpu.VMEM(source.shape, BF16),
            pltpu.VMEM((5, 1, C), F32),
            pltpu.SemaphoreType.DMA((7,)),
        ],
        compiler_params=pltpu.CompilerParams(vmem_limit_bytes=67043328),
        cost_estimate=cost(1),
    )(weight_one, source, *vectors)
    kernel_one = exchange(packed, COL)
    other = lax.ppermute(source, "yl", [(0, 1), (1, 0)])
    near = [p for x in range(3) for p in ((4 * x + 3, 4 * x + 4), (4 * x + 4, 4 * x + 3))]
    far = [p for x in range(3) for p in ((4 * x + 3, 4 * x + 6), (4 * x + 4, 4 * x + 1))]
    near = lax.ppermute(source, COL, near)
    far = lax.ppermute(source, COL, far)
    joined = call(join_kernel, (source, other, near, far), sds((3, T, 4, 4, C), BF16), cost=cost(1))
    wide = lax.all_gather(joined, "core", axis=0, tiled=False)
    kernel_two = [weight_two]
    for step in range(1, 4):
        kernel_two.append(lax.ppermute(weight_two, "x", [(x, (x + step) % 4) for x in range(4)]))
    hidden, stats = call(
        conv_one_kernel,
        (wide, kernel_one, vec),
        (sds((4, T, ROW, 128), BF16), sds((4, 8, 128), F32)),
        (pltpu.VMEM((4, T + 2, ROW, C), BF16), pltpu.VMEM((9, C, C), BF16)),
        cost=cost(4),
    )
    intersections, stats = lax.optimization_barrier((intersections, stats))
    stats = exchange(stats, "x")
    shared = pl.pallas_call(
        count_kernel,
        out_shape=sds((1, C), F32),
        in_specs=[pl.BlockSpec(memory_space=pltpu.SMEM)],
        out_specs=whole(),
    )(intersections)
    home, away = call(
        conv_two_kernel,
        (hidden, stats, *kernel_two, vec),
        (sds((2, T, 4, 4, C), F32), sds((2, T, 4, 4, C), BF16)),
        (pltpu.VMEM((4, T + 2, 16, C), BF16), pltpu.VMEM((9, C, C), BF16)),
        cost=cost(4),
    )
    got = lax.all_gather(away, "core", axis=0, tiled=False)
    own, rest_tail, rest = call(
        pair_kernel,
        (home, got),
        (sds((T, 4, 4, C), F32), sds((OVMAX, 4, 4, C), BF16), sds((T - OVMAX, 4, 4, C), BF16)),
        cost=cost(1),
    )
    swap = [(0, 1), (1, 0)]
    rest_tail = lax.ppermute(rest_tail, "yl", swap)
    rest = lax.ppermute(rest, "yl", swap)
    tail = call(tail_kernel, (own, rest_tail, source, vec), sds((OVMAX, 4, 4, C), BF16), cost=cost(1))
    tiles = lax.axis_size(TILE)
    received = lax.ppermute(tail, TILE, [(i, i + 1) for i in range(tiles - 1)])
    out = call(blend_kernel, (own, rest, tail, source, vec, shared, received), sds((T, 4, 4, C), BF16), cost=cost(1))
    return out[None]


def solution(mesh):
    wide = Mesh(mesh.devices.reshape(8, 4, 4, 2, 2), ("z", "yh", "x", "yl", "core"))
    image = P(TILE, None, None, COL, None)
    kernel = P(None, None, None, COL, None)
    in_specs = (image, P(TILE), P(), P(), kernel, P(), P(), kernel, P())
    return jax.shard_map(block, mesh=wide, in_specs=in_specs, out_specs=image, check_vma=False)
```

```python
import jax
import jax.numpy as jnp
from jax import lax
from jax.experimental import pallas as pl
from jax.experimental.pallas import tpu as pltpu
from jax.sharding import Mesh
from jax.sharding import PartitionSpec as P

GROUPS = 32
OVMAX = 4
epsilon = 1e-06
F32, BF16 = jnp.float32, jnp.bfloat16

COL = ("x", "yl", "core")
TILE = ("z", "yh")
T, H, W, C = 17, 4, 64, 256
ROW = 24
PARAMS = pltpu.CompilerParams(vmem_limit_bytes=48 * 1024 * 1024)


def whole():
    return pl.BlockSpec(memory_space=pltpu.VMEM)


def call(kernel, inputs, out_shape, scratch=(), cost=None):
    return pl.pallas_call(
        kernel,
        out_shape=out_shape,
        in_specs=[whole()] * len(inputs),
        out_specs=jax.tree.map(lambda _: whole(), out_shape),
        scratch_shapes=list(scratch),
        compiler_params=PARAMS,
        cost_estimate=cost,
    )(*inputs)


def cost(us):
    return pl.CostEstimate(flops=int(us * 4e8), bytes_accessed=1 << 20, transcendentals=0)


def lanes(shape):
    return lax.broadcasted_iota(jnp.int32, shape, len(shape) - 1)


def rows(shape):
    return lax.broadcasted_iota(jnp.int32, shape, len(shape) - 2)


def split3(value):
    high = value.astype(BF16)
    rest = value - high.astype(F32)
    middle = rest.astype(BF16)
    return high, middle, (rest - middle.astype(F32)).astype(BF16)


def group_sum(value):
    lane, width = lanes(value.shape), value.shape[1]
    for k in (1, 2, 4):
        up, down = pltpu.roll(value, k, 1), pltpu.roll(value, width - k, 1)
        value = value + jnp.where((lane & k) != 0, up, down)
    return value


def moments(total, squares):
    members = T * H * W * (C // GROUPS)
    mean = total / members
    spread = jnp.maximum(squares / members - mean * mean, 0.0)
    return mean, lax.rsqrt(spread + epsilon)


def silu(v):
    return v * (0.5 * jnp.tanh(0.5 * v) + 0.5)


def pack_kernel(
    w_hbm, latent_hbm, g1, s1, g2, s2, b, out_ref, vec_ref, w_ref, latent_ref, line, sems
):
    copies = [
        pltpu.make_async_copy(source, target, sems.at[i])
        for i, (source, target) in enumerate(
            [(latent_hbm, latent_ref), (w_hbm, w_ref)]
            + [(source, line.at[i]) for i, source in enumerate((g1, s1, g2, s2, b))]
        )
    ]
    for copy in copies:
        copy.start()
    for copy in copies:
        copy.wait()
    for i in range(5):
        vec_ref[i : i + 1] = line[i]
    vec_ref[5:8] = jnp.zeros((3, C), F32)
    totals, powers = [], []
    for h in range(H):
        total, squares = jnp.zeros((4, C), F32), jnp.zeros((4, C), F32)
        for t in range(T):
            v = latent_ref[t, h].astype(F32)
            total += v
            squares += v * v
        totals.append(total)
        powers.append(squares)
    total = (totals[0] + totals[1]) + (totals[2] + totals[3])
    squares = (powers[0] + powers[1]) + (powers[2] + powers[3])
    line_sum = jnp.broadcast_to(jnp.sum(total, axis=0, keepdims=True), (8, C))
    line_square = jnp.broadcast_to(jnp.sum(squares, axis=0, keepdims=True), (8, C))
    spot = lanes((8, C)) & 7
    sums = jnp.zeros((8, C), F32)
    for start, value in ((0, group_sum(line_sum)), (3, group_sum(line_square))):
        for i, piece in enumerate(split3(value)):
            sums = jnp.where(spot == start + i, piece.astype(F32), sums)
    halves = [sums[0:1, 0:128], sums[0:1, 128:256]]
    extra = jnp.concatenate(
        [pltpu.roll(sums[:, 0:128], 64, 1)[0:1], halves[0], pltpu.roll(sums[:, 128:256], 64, 1)[0:1], halves[1],
         jnp.zeros((12, 128), F32)],
        axis=0,
    )
    row, col = rows((C, C)), lanes((C, C))
    source = 64 * ((col // 16) % 4) + 16 * (col // 64) + col % 16
    swapped = col ^ 64
    other = 64 * ((swapped // 16) % 4) + 16 * (swapped // 64) + swapped % 16
    left = lanes((16, 128)) < 64
    w = w_ref[...].reshape(27 * 16, C)
    same = jnp.dot(w, (row == source).astype(BF16), preferred_element_type=F32)
    swap = jnp.dot(w, (row == other).astype(BF16), preferred_element_type=F32)

    def block(array, k, dw, j):
        dt, dh = k % 3, k // 3
        at = ((dt * 3 + dh) * 3 + dw) * 16
        return array[at : at + 16, 128 * (j // 2) : 128 * (j // 2) + 128]

    for j in range(4):
        first, second = (same, swap) if j % 2 == 0 else (swap, same)
        for m in range(14):
            if m < 9:
                a, b = block(first, m, 0, j), block(second, m, 1, j)
            else:
                a = block(first, m - 9, 2, j)
                b = block(second, m - 4, 2, j) if m < 13 else extra
            tile = jnp.where(left, a, b).astype(BF16)
            for x in range(4):
                out_ref[4 * x + j, m] = tile


def count_kernel(n_ref, out_ref):
    out_ref[...] = jnp.full((1, C), n_ref[0], jnp.int32).astype(F32)


def join_kernel(latent_ref, other_ref, near_ref, far_ref, out_ref):
    out_ref[0] = latent_ref[...]
    out_ref[1] = other_ref[...]
    straight = lax.axis_index("yl") == lax.axis_index("core")

    @pl.when(straight)
    def _():
        out_ref[2] = near_ref[...]

    @pl.when(jnp.logical_not(straight))
    def _():
        out_ref[2] = far_ref[...]


def conv_one_kernel(l_ref, w_ref, vec_ref, hid_ref, st_ref, act, wm):
    me = lax.axis_index("x")
    left = lanes((16, 128)) < 64
    nothing = jnp.zeros((16, 128), BF16)
    for p in range(16):
        for k in range(9):
            wm[k, 16 * p : 16 * p + 16, 0:128] = w_ref[p, k]
            if k < 5:
                last = jnp.where(left, w_ref[p, 9 + k], nothing)
            else:
                last = jnp.where(left, nothing, w_ref[p, 4 + k])
            wm[k, 16 * p : 16 * p + 16, 128:256] = last
    sums = sum(w_ref[p, 13].astype(F32) for p in range(16))[0:8]
    turned = pltpu.roll(sums, 64, 1)
    first = lanes((1, 128)) < 64
    line = jnp.concatenate(
        [jnp.where(first, turned[2 * i : 2 * i + 1], sums[2 * i + 1 : 2 * i + 2]) for i in range(2)], axis=1
    )
    line = jnp.broadcast_to(line, (8, C))
    spot = lanes((8, C)) & 7
    mean, inv = moments(
        group_sum(jnp.where(spot < 3, line, 0.0)), group_sum(jnp.where((spot > 2) & (spot < 6), line, 0.0))
    )
    scale = inv * vec_ref[0:1]
    mean, scale = mean[0:1], scale[0:1]
    shift = vec_ref[1:2]
    yl = lax.axis_index("yl")
    slots = (yl, 1 - yl)
    row = rows((ROW, C))
    inside = (row >= jnp.where(me == 0, 4, 0)) & (row < jnp.where(me == 3, 20, ROW))
    act[:, 0:2] = jnp.zeros((4, 2, ROW, C), BF16)

    def frame(t, _):
        for h in range(4):
            lo = l_ref[0, 2, t, h].astype(F32)
            hi = l_ref[1, 2, t, h].astype(F32)
            own = [l_ref[q % 2, slots[q // 2], t, h].astype(F32) for q in range(4)]
            v = jnp.concatenate([lo, *own, hi], axis=0)
            y = silu((v - mean) * scale + shift)
            act[h, t + 2] = jnp.where(inside, y, 0.0).astype(BF16)
        return 0

    lax.fori_loop(0, T, frame, 0)

    size = T * ROW
    lane = lanes((size, 128))
    place = rows((size, 128)) % ROW
    own = (place >= 4) & (place < 20)
    s1, s2 = jnp.zeros((1, 128), F32), jnp.zeros((1, 128), F32)
    for h in range(4):
        taps = [dh for dh in range(3) if 0 <= h + dh - 1 < 4]
        lhs = jnp.concatenate(
            [act[h + dh - 1, dt : dt + T].reshape(size, C) for dh in taps for dt in range(3)], axis=1
        )
        rhs = wm[3 * taps[0] : 3 * taps[-1] + 3].reshape(-1, C)
        y = jnp.dot(lhs, rhs, preferred_element_type=F32)
        y0, y1 = y[:, 0:128], y[:, 128:256]
        z = jnp.where(lane < 64, pltpu.roll(y0, 1, 0), y0) + pltpu.roll(y1, size - 1, 0)
        hidden = (z + pltpu.roll(z, 64, 1)).astype(BF16)
        hid_ref[h] = hidden.reshape(T, ROW, 128)
        counted = jnp.where(own, hidden.astype(F32), 0.0)
        s1 += jnp.sum(counted, axis=0, keepdims=True)
        s2 += jnp.sum(counted * counted, axis=0, keepdims=True)
    stats = jnp.concatenate([s1, s2, jnp.zeros((6, 128), F32)], axis=0)
    for d in range(4):
        st_ref[d] = stats


def conv_two_kernel(hid_ref, st_ref, w0_ref, w1_ref, w2_ref, w3_ref, vec_ref, home_ref, away_ref, act, wm):
    me = lax.axis_index("x")
    j = 2 * lax.axis_index("yl") + lax.axis_index("core")
    for step, w_ref in enumerate((w0_ref, w1_ref, w2_ref, w3_ref)):
        x = lax.rem(me + 4 - step, 4)
        for k in range(9):
            for dw in range(3):
                at = pl.multiple_of(64 * dw + 16 * x, 16)
                wm[k, pl.ds(at, 16)] = w_ref[k % 3, k // 3, dw]
    for k in range(9):
        wm[k, 192:256] = jnp.zeros((64, C), BF16)
    stats = st_ref[0] + st_ref[1] + st_ref[2] + st_ref[3]
    mean, inv = moments(
        group_sum(jnp.broadcast_to(stats[0:1], (8, 128))), group_sum(jnp.broadcast_to(stats[1:2], (8, 128)))
    )
    row, lane = rows((C, 128)), lanes((C, 128))
    mine = (row == 64 * ((lane // 16) % 4) + 16 * j + lane % 16).astype(F32)
    picked = jnp.dot(vec_ref[...], mine, precision=lax.Precision.HIGHEST, preferred_element_type=F32)
    scale, shift = inv[0:1] * picked[2:3], picked[3:4]
    mean = mean[0:1]
    row = rows((ROW, 128))
    inside = (row >= jnp.where(me == 0, 4, 0)) & (row < jnp.where(me == 3, 20, ROW))
    left = lanes((16, 128)) < 64
    place = jnp.full((8, 128), j, jnp.int32)
    odd, upper = (place & 1) != 0, (place & 2) != 0
    act[:, 0:2] = jnp.zeros((4, 2, 16, C), BF16)

    def frame(t, _):
        for h in range(4):
            v = hid_ref[h, t].astype(F32)
            y = silu((v - mean) * scale + shift)
            y = jnp.where(inside, y, 0.0)
            a0, a1, a2 = (pltpu.roll(y, ROW - 3 - dw, 0)[0:16] for dw in range(3))
            for at, tile in ((0, jnp.where(left, a0, a1)), (128, jnp.where(left, a2, 0.0))):
                low, high = jnp.where(upper, tile[8:16], tile[0:8]), jnp.where(upper, tile[0:8], tile[8:16])
                low = jnp.where(odd, pltpu.roll(low, 4, 0), low)
                high = jnp.where(odd, pltpu.roll(high, 4, 0), high)
                act[h, t + 2, :, at : at + 128] = jnp.concatenate([low, high], axis=0).astype(BF16)
        return 0

    lax.fori_loop(0, T, frame, 0)
    for h in range(4):
        taps = [dh for dh in range(3) if 0 <= h + dh - 1 < 4]
        lhs = jnp.concatenate(
            [act[h + dh - 1, dt : dt + T].reshape(T * 16, C) for dh in taps for dt in range(3)], axis=1
        )
        rhs = wm[3 * taps[0] : 3 * taps[-1] + 3].reshape(-1, C)
        y = jnp.dot(lhs, rhs, preferred_element_type=F32).reshape(T, 16, C)
        for d in range(4):
            target = away_ref if d % 2 else home_ref
            target[d // 2, :, h] = y[:, 4 * d : 4 * d + 4].astype(target.dtype)


def pair_kernel(home_ref, got_ref, latent_ref, vec_ref, own_ref, send_ref, straight_ref, across_ref):
    other = 1 - lax.axis_index("core")
    for t in range(T):
        own = home_ref[0, t] + got_ref[other, 0, t].astype(F32)
        send = (home_ref[1, t] + got_ref[other, 1, t].astype(F32)).astype(BF16)
        own = latent_ref[t].astype(F32) + (own + vec_ref[4:5])
        own_ref[t] = own
        send_ref[t] = send
        if t >= T - OVMAX:
            straight_ref[t - T + OVMAX] = own.astype(BF16)
            across_ref[t - T + OVMAX] = send


def blend_kernel(own_ref, other_ref, shared_ref, straight_ref, across_ref, out_ref):
    shared = shared_ref[...]
    before = [
        (straight_ref[i].astype(F32) + across_ref[i].astype(F32)).astype(BF16).astype(F32) for i in range(OVMAX)
    ]
    for t in range(T):
        own = (own_ref[t] + other_ref[t].astype(F32)).astype(BF16)
        if t < OVMAX:
            other = before[OVMAX - 1]
            for n in range(t + 2, OVMAX + 1):
                other = jnp.where((shared == n)[None], before[OVMAX - n + t], other)
            share = jnp.full((1, C), t + 1, F32) / (shared + 1.0)
            head = own.astype(F32)
            mixed = share * head + (1.0 - share) * other
            own = jnp.where((shared > t)[None], mixed, head).astype(BF16)
        out_ref[t] = own


def exchange(array, axis):
    return lax.all_to_all(array, axis, split_axis=0, concat_axis=0, tiled=True)


def block(latent, intersections, gain_one, shift_one, weight_one, gain_two, shift_two, weight_two, bias):
    source = latent[0]
    flat = lambda v: v.reshape(1, C)
    sds = jax.ShapeDtypeStruct
    vectors = tuple(flat(v) for v in (gain_one, shift_one, gain_two, shift_two, bias))
    packed, vec = pl.pallas_call(
        pack_kernel,
        out_shape=(sds((16, 14, 16, 128), BF16), sds((8, C), F32)),
        in_specs=[pl.BlockSpec(memory_space=pl.ANY)] * 7,
        out_specs=(whole(), whole()),
        scratch_shapes=[
            pltpu.VMEM(weight_one.shape, BF16),
            pltpu.VMEM(source.shape, BF16),
            pltpu.VMEM((5, 1, C), F32),
            pltpu.SemaphoreType.DMA((7,)),
        ],
        compiler_params=pltpu.CompilerParams(vmem_limit_bytes=67043328),
        cost_estimate=cost(1),
    )(weight_one, source, *vectors)
    kernel_one = exchange(packed, COL)
    other = lax.ppermute(source, "yl", [(0, 1), (1, 0)])
    near = [p for x in range(3) for p in ((4 * x + 3, 4 * x + 4), (4 * x + 4, 4 * x + 3))]
    far = [p for x in range(3) for p in ((4 * x + 3, 4 * x + 6), (4 * x + 4, 4 * x + 1))]
    near = lax.ppermute(source, COL, near)
    far = lax.ppermute(source, COL, far)
    joined = call(join_kernel, (source, other, near, far), sds((3, T, 4, 4, C), BF16), cost=cost(1))
    wide = lax.all_gather(joined, "core", axis=0, tiled=False)
    kernel_two = [weight_two]
    for step in range(1, 4):
        kernel_two.append(lax.ppermute(weight_two, "x", [(x, (x + step) % 4) for x in range(4)]))
    hidden, stats = call(
        conv_one_kernel,
        (wide, kernel_one, vec),
        (sds((4, T, ROW, 128), BF16), sds((4, 8, 128), F32)),
        (pltpu.VMEM((4, T + 2, ROW, C), BF16), pltpu.VMEM((9, C, C), BF16)),
        cost=cost(4),
    )
    intersections, stats = lax.optimization_barrier((intersections, stats))
    stats = exchange(stats, "x")
    shared = pl.pallas_call(
        count_kernel,
        out_shape=sds((1, C), F32),
        in_specs=[pl.BlockSpec(memory_space=pltpu.SMEM)],
        out_specs=whole(),
    )(intersections)
    home, away = call(
        conv_two_kernel,
        (hidden, stats, *kernel_two, vec),
        (sds((2, T, 4, 4, C), F32), sds((2, T, 4, 4, C), BF16)),
        (pltpu.VMEM((4, T + 2, 16, C), BF16), pltpu.VMEM((9, C, C), BF16)),
        cost=cost(4),
    )
    got = lax.all_gather(away, "core", axis=0, tiled=False)
    own, send, straight, across = call(
        pair_kernel,
        (home, got, source, vec),
        (sds((T, 4, 4, C), F32), sds((T, 4, 4, C), BF16), sds((OVMAX, 4, 4, C), BF16), sds((OVMAX, 4, 4, C), BF16)),
        cost=cost(1),
    )
    tiles = lax.axis_size(TILE)
    rest = lax.ppermute(send, "yl", [(0, 1), (1, 0)])
    straight = lax.ppermute(straight, TILE, [(i, i + 1) for i in range(tiles - 1)])
    route = [(2 * i + yl, 2 * i + 3 - yl) for i in range(tiles - 1) for yl in range(2)]
    across = lax.ppermute(across, ("z", "yh", "yl"), route)
    out = call(blend_kernel, (own, rest, shared, straight, across), sds((T, 4, 4, C), BF16), cost=cost(1))
    return out[None]


def solution(mesh):
    wide = Mesh(mesh.devices.reshape(8, 4, 4, 2, 2), ("z", "yh", "x", "yl", "core"))
    image = P(TILE, None, None, COL, None)
    kernel = P(None, None, None, COL, None)
    in_specs = (image, P(TILE), P(), P(), kernel, P(), P(), kernel, P())
    return jax.shard_map(block, mesh=wide, in_specs=in_specs, out_specs=image, check_vma=False)
```

```python
import jax
import jax.numpy as jnp
from jax import lax
from jax.experimental import pallas as pl
from jax.experimental.pallas import tpu as pltpu
from jax.sharding import Mesh
from jax.sharding import PartitionSpec as P

GROUPS = 32
OVMAX = 4
epsilon = 1e-06
F32, BF16 = jnp.float32, jnp.bfloat16

COL = ("x", "yl", "core")
TILE = ("z", "yh")
T, H, W, C = 17, 4, 64, 256
ROW = 24
PARAMS = pltpu.CompilerParams(vmem_limit_bytes=48 * 1024 * 1024)


def whole():
    return pl.BlockSpec(memory_space=pltpu.VMEM)


def call(kernel, inputs, out_shape, scratch=(), cost=None):
    return pl.pallas_call(
        kernel,
        out_shape=out_shape,
        in_specs=[whole()] * len(inputs),
        out_specs=jax.tree.map(lambda _: whole(), out_shape),
        scratch_shapes=list(scratch),
        compiler_params=PARAMS,
        cost_estimate=cost,
    )(*inputs)


def cost(us):
    return pl.CostEstimate(flops=int(us * 4e8), bytes_accessed=1 << 20, transcendentals=0)


def lanes(shape):
    return lax.broadcasted_iota(jnp.int32, shape, len(shape) - 1)


def rows(shape):
    return lax.broadcasted_iota(jnp.int32, shape, len(shape) - 2)


def split3(value):
    high = value.astype(BF16)
    rest = value - high.astype(F32)
    middle = rest.astype(BF16)
    return high, middle, (rest - middle.astype(F32)).astype(BF16)


def group_sum(value):
    lane, width = lanes(value.shape), value.shape[1]
    for k in (1, 2, 4):
        up, down = pltpu.roll(value, k, 1), pltpu.roll(value, width - k, 1)
        value = value + jnp.where((lane & k) != 0, up, down)
    return value


def moments(total, squares):
    members = T * H * W * (C // GROUPS)
    mean = total / members
    spread = jnp.maximum(squares / members - mean * mean, 0.0)
    return mean, lax.rsqrt(spread + epsilon)


def silu(v):
    return v * (0.5 * jnp.tanh(0.5 * v) + 0.5)


def pack_kernel(
    w_hbm, latent_hbm, g1, s1, g2, s2, b, out_ref, vec_ref, w_ref, latent_ref, line, sems
):
    copies = [
        pltpu.make_async_copy(source, target, sems.at[i])
        for i, (source, target) in enumerate(
            [(latent_hbm, latent_ref), (w_hbm, w_ref)]
            + [(source, line.at[i]) for i, source in enumerate((g1, s1, g2, s2, b))]
        )
    ]
    for copy in copies:
        copy.start()
    for copy in copies:
        copy.wait()
    for i in range(5):
        vec_ref[i : i + 1] = line[i]
    vec_ref[5:8] = jnp.zeros((3, C), F32)
    totals, powers = [], []
    for h in range(H):
        total, squares = jnp.zeros((4, C), F32), jnp.zeros((4, C), F32)
        for t in range(T):
            v = latent_ref[t, h].astype(F32)
            total += v
            squares += v * v
        totals.append(total)
        powers.append(squares)
    total = (totals[0] + totals[1]) + (totals[2] + totals[3])
    squares = (powers[0] + powers[1]) + (powers[2] + powers[3])
    line_sum = jnp.broadcast_to(jnp.sum(total, axis=0, keepdims=True), (8, C))
    line_square = jnp.broadcast_to(jnp.sum(squares, axis=0, keepdims=True), (8, C))
    spot = lanes((8, C)) & 7
    sums = jnp.zeros((8, C), F32)
    for start, value in ((0, group_sum(line_sum)), (3, group_sum(line_square))):
        for i, piece in enumerate(split3(value)):
            sums = jnp.where(spot == start + i, piece.astype(F32), sums)
    halves = [sums[0:1, 0:128], sums[0:1, 128:256]]
    extra = jnp.concatenate(
        [pltpu.roll(sums[:, 0:128], 64, 1)[0:1], halves[0], pltpu.roll(sums[:, 128:256], 64, 1)[0:1], halves[1],
         jnp.zeros((12, 128), F32)],
        axis=0,
    )
    row, col = rows((C, C)), lanes((C, C))
    source = 64 * ((col // 16) % 4) + 16 * (col // 64) + col % 16
    swapped = col ^ 64
    other = 64 * ((swapped // 16) % 4) + 16 * (swapped // 64) + swapped % 16
    left = lanes((16, 128)) < 64
    w = w_ref[...].reshape(27 * 16, C)
    same = jnp.dot(w, (row == source).astype(BF16), preferred_element_type=F32)
    swap = jnp.dot(w, (row == other).astype(BF16), preferred_element_type=F32)

    def block(array, k, dw, j):
        dt, dh = k % 3, k // 3
        at = ((dt * 3 + dh) * 3 + dw) * 16
        return array[at : at + 16, 128 * (j // 2) : 128 * (j // 2) + 128]

    for j in range(4):
        first, second = (same, swap) if j % 2 == 0 else (swap, same)
        for m in range(14):
            if m < 9:
                a, b = block(first, m, 0, j), block(second, m, 1, j)
            else:
                a = block(first, m - 9, 2, j)
                b = block(second, m - 4, 2, j) if m < 13 else extra
            tile = jnp.where(left, a, b).astype(BF16)
            for x in range(4):
                out_ref[4 * x + j, m] = tile


def count_kernel(n_ref, out_ref):
    out_ref[...] = jnp.full((1, C), n_ref[0], jnp.int32).astype(F32)


def join_kernel(latent_ref, other_ref, near_ref, far_ref, out_ref):
    out_ref[0] = latent_ref[...]
    out_ref[1] = other_ref[...]
    straight = lax.axis_index("yl") == lax.axis_index("core")

    @pl.when(straight)
    def _():
        out_ref[2] = near_ref[...]

    @pl.when(jnp.logical_not(straight))
    def _():
        out_ref[2] = far_ref[...]


def conv_one_kernel(l_ref, w_ref, vec_ref, hid_ref, st_ref, act, wm):
    me = lax.axis_index("x")
    left = lanes((16, 128)) < 64
    nothing = jnp.zeros((16, 128), BF16)
    for p in range(16):
        for k in range(9):
            wm[k, 16 * p : 16 * p + 16, 0:128] = w_ref[p, k]
            if k < 5:
                last = jnp.where(left, w_ref[p, 9 + k], nothing)
            else:
                last = jnp.where(left, nothing, w_ref[p, 4 + k])
            wm[k, 16 * p : 16 * p + 16, 128:256] = last
    sums = sum(w_ref[p, 13].astype(F32) for p in range(16))[0:8]
    turned = pltpu.roll(sums, 64, 1)
    first = lanes((1, 128)) < 64
    line = jnp.concatenate(
        [jnp.where(first, turned[2 * i : 2 * i + 1], sums[2 * i + 1 : 2 * i + 2]) for i in range(2)], axis=1
    )
    line = jnp.broadcast_to(line, (8, C))
    spot = lanes((8, C)) & 7
    mean, inv = moments(
        group_sum(jnp.where(spot < 3, line, 0.0)), group_sum(jnp.where((spot > 2) & (spot < 6), line, 0.0))
    )
    scale = inv * vec_ref[0:1]
    mean, scale = mean[0:1], scale[0:1]
    shift = vec_ref[1:2]
    yl = lax.axis_index("yl")
    slots = (yl, 1 - yl)
    row = rows((ROW, C))
    inside = (row >= jnp.where(me == 0, 4, 0)) & (row < jnp.where(me == 3, 20, ROW))
    act[:, 0:2] = jnp.zeros((4, 2, ROW, C), BF16)

    def frame(t):
        for h in range(4):
            lo = l_ref[0, 2, t, h].astype(F32)
            hi = l_ref[1, 2, t, h].astype(F32)
            own = [l_ref[q % 2, slots[q // 2], t, h].astype(F32) for q in range(4)]
            v = jnp.concatenate([lo, *own, hi], axis=0)
            y = silu((v - mean) * scale + shift)
            act[h, t + 2] = jnp.where(inside, y, 0.0).astype(BF16)
        return 0

    for t in range(T):
        frame(t)

    size = T * ROW
    lane = lanes((size, 128))
    place = rows((size, 128)) % ROW
    own = (place >= 4) & (place < 20)
    s1, s2 = jnp.zeros((1, 128), F32), jnp.zeros((1, 128), F32)
    for h in range(4):
        taps = [dh for dh in range(3) if 0 <= h + dh - 1 < 4]
        lhs = jnp.concatenate(
            [act[h + dh - 1, dt : dt + T].reshape(size, C) for dh in taps for dt in range(3)], axis=1
        )
        rhs = wm[3 * taps[0] : 3 * taps[-1] + 3].reshape(-1, C)
        y = jnp.dot(lhs, rhs, preferred_element_type=F32)
        y0, y1 = y[:, 0:128], y[:, 128:256]
        z = jnp.where(lane < 64, pltpu.roll(y0, 1, 0), y0) + pltpu.roll(y1, size - 1, 0)
        hidden = (z + pltpu.roll(z, 64, 1)).astype(BF16)
        hid_ref[h] = hidden.reshape(T, ROW, 128)
        counted = jnp.where(own, hidden.astype(F32), 0.0)
        s1 += jnp.sum(counted, axis=0, keepdims=True)
        s2 += jnp.sum(counted * counted, axis=0, keepdims=True)
    stats = jnp.concatenate([s1, s2, jnp.zeros((6, 128), F32)], axis=0)
    for d in range(4):
        st_ref[d] = stats


def conv_two_kernel(hid_ref, st_ref, w0_ref, w1_ref, w2_ref, w3_ref, vec_ref, home_ref, away_ref, act, wm):
    me = lax.axis_index("x")
    j = 2 * lax.axis_index("yl") + lax.axis_index("core")
    for step, w_ref in enumerate((w0_ref, w1_ref, w2_ref, w3_ref)):
        x = lax.rem(me + 4 - step, 4)
        for k in range(9):
            for dw in range(3):
                at = pl.multiple_of(64 * dw + 16 * x, 16)
                wm[k, pl.ds(at, 16)] = w_ref[k % 3, k // 3, dw]
    for k in range(9):
        wm[k, 192:256] = jnp.zeros((64, C), BF16)
    stats = st_ref[0] + st_ref[1] + st_ref[2] + st_ref[3]
    mean, inv = moments(
        group_sum(jnp.broadcast_to(stats[0:1], (8, 128))), group_sum(jnp.broadcast_to(stats[1:2], (8, 128)))
    )
    row, lane = rows((C, 128)), lanes((C, 128))
    mine = (row == 64 * ((lane // 16) % 4) + 16 * j + lane % 16).astype(F32)
    picked = jnp.dot(vec_ref[...], mine, precision=lax.Precision.HIGHEST, preferred_element_type=F32)
    scale, shift = inv[0:1] * picked[2:3], picked[3:4]
    mean = mean[0:1]
    row = rows((ROW, 128))
    inside = (row >= jnp.where(me == 0, 4, 0)) & (row < jnp.where(me == 3, 20, ROW))
    left = lanes((16, 128)) < 64
    place = jnp.full((8, 128), j, jnp.int32)
    odd, upper = (place & 1) != 0, (place & 2) != 0
    act[:, 0:2] = jnp.zeros((4, 2, 16, C), BF16)

    def frame(t):
        for h in range(4):
            v = hid_ref[h, t].astype(F32)
            y = silu((v - mean) * scale + shift)
            y = jnp.where(inside, y, 0.0)
            a0, a1, a2 = (pltpu.roll(y, ROW - 3 - dw, 0)[0:16] for dw in range(3))
            for at, tile in ((0, jnp.where(left, a0, a1)), (128, jnp.where(left, a2, 0.0))):
                low, high = jnp.where(upper, tile[8:16], tile[0:8]), jnp.where(upper, tile[0:8], tile[8:16])
                low = jnp.where(odd, pltpu.roll(low, 4, 0), low)
                high = jnp.where(odd, pltpu.roll(high, 4, 0), high)
                act[h, t + 2, :, at : at + 128] = jnp.concatenate([low, high], axis=0).astype(BF16)
        return 0

    for t in range(T):
        frame(t)
    for h in range(4):
        taps = [dh for dh in range(3) if 0 <= h + dh - 1 < 4]
        lhs = jnp.concatenate(
            [act[h + dh - 1, dt : dt + T].reshape(T * 16, C) for dh in taps for dt in range(3)], axis=1
        )
        rhs = wm[3 * taps[0] : 3 * taps[-1] + 3].reshape(-1, C)
        y = jnp.dot(lhs, rhs, preferred_element_type=F32).reshape(T, 16, C)
        for d in range(4):
            target = away_ref if d % 2 else home_ref
            target[d // 2, :, h] = y[:, 4 * d : 4 * d + 4].astype(target.dtype)


def pair_kernel(home_ref, got_ref, own_ref, tail_ref, main_ref):
    other = 1 - lax.axis_index("core")
    for t in range(T):
        own_ref[t] = home_ref[0, t] + got_ref[other, 0, t].astype(F32)
        send = (home_ref[1, t] + got_ref[other, 1, t].astype(F32)).astype(BF16)
        if t < T - OVMAX:
            main_ref[t] = send
        else:
            tail_ref[t - T + OVMAX] = send


def decode(own, other, latent, bias):
    return (latent.astype(F32) + (own + other.astype(F32) + bias)).astype(BF16)


def tail_kernel(own_ref, other_ref, latent_ref, vec_ref, tail_ref):
    for i in range(OVMAX):
        t = T - OVMAX + i
        tail_ref[i] = decode(own_ref[t], other_ref[i], latent_ref[t], vec_ref[4:5])


def blend_kernel(own_ref, other_ref, tail_ref, latent_ref, vec_ref, shared_ref, received_ref, out_ref):
    bias, shared = vec_ref[4:5], shared_ref[...]
    for t in range(T):
        if t >= T - OVMAX:
            out_ref[t] = tail_ref[t - T + OVMAX]
            continue
        own = decode(own_ref[t], other_ref[t], latent_ref[t], bias)
        if t < OVMAX:
            other = received_ref[OVMAX - 1].astype(F32)
            for n in range(t + 2, OVMAX + 1):
                other = jnp.where((shared == n)[None], received_ref[OVMAX - n + t].astype(F32), other)
            share = jnp.full((1, C), t + 1, F32) / (shared + 1.0)
            head = own.astype(F32)
            mixed = share * head + (1.0 - share) * other
            own = jnp.where((shared > t)[None], mixed, head).astype(BF16)
        out_ref[t] = own


def exchange(array, axis):
    return lax.all_to_all(array, axis, split_axis=0, concat_axis=0, tiled=True)


def block(latent, intersections, gain_one, shift_one, weight_one, gain_two, shift_two, weight_two, bias):
    source = latent[0]
    flat = lambda v: v.reshape(1, C)
    sds = jax.ShapeDtypeStruct
    vectors = tuple(flat(v) for v in (gain_one, shift_one, gain_two, shift_two, bias))
    packed, vec = pl.pallas_call(
        pack_kernel,
        out_shape=(sds((16, 14, 16, 128), BF16), sds((8, C), F32)),
        in_specs=[pl.BlockSpec(memory_space=pl.ANY)] * 7,
        out_specs=(whole(), whole()),
        scratch_shapes=[
            pltpu.VMEM(weight_one.shape, BF16),
            pltpu.VMEM(source.shape, BF16),
            pltpu.VMEM((5, 1, C), F32),
            pltpu.SemaphoreType.DMA((7,)),
        ],
        compiler_params=pltpu.CompilerParams(vmem_limit_bytes=67043328),
        cost_estimate=cost(1),
    )(weight_one, source, *vectors)
    kernel_one = exchange(packed, COL)
    other = lax.ppermute(source, "yl", [(0, 1), (1, 0)])
    near = [p for x in range(3) for p in ((4 * x + 3, 4 * x + 4), (4 * x + 4, 4 * x + 3))]
    far = [p for x in range(3) for p in ((4 * x + 3, 4 * x + 6), (4 * x + 4, 4 * x + 1))]
    near = lax.ppermute(source, COL, near)
    far = lax.ppermute(source, COL, far)
    joined = call(join_kernel, (source, other, near, far), sds((3, T, 4, 4, C), BF16), cost=cost(1))
    wide = lax.all_gather(joined, "core", axis=0, tiled=False)
    kernel_two = [weight_two]
    for step in range(1, 4):
        kernel_two.append(lax.ppermute(weight_two, "x", [(x, (x + step) % 4) for x in range(4)]))
    hidden, stats = call(
        conv_one_kernel,
        (wide, kernel_one, vec),
        (sds((4, T, ROW, 128), BF16), sds((4, 8, 128), F32)),
        (pltpu.VMEM((4, T + 2, ROW, C), BF16), pltpu.VMEM((9, C, C), BF16)),
        cost=cost(4),
    )
    intersections, stats = lax.optimization_barrier((intersections, stats))
    stats = exchange(stats, "x")
    shared = pl.pallas_call(
        count_kernel,
        out_shape=sds((1, C), F32),
        in_specs=[pl.BlockSpec(memory_space=pltpu.SMEM)],
        out_specs=whole(),
    )(intersections)
    home, away = call(
        conv_two_kernel,
        (hidden, stats, *kernel_two, vec),
        (sds((2, T, 4, 4, C), F32), sds((2, T, 4, 4, C), BF16)),
        (pltpu.VMEM((4, T + 2, 16, C), BF16), pltpu.VMEM((9, C, C), BF16)),
        cost=cost(4),
    )
    got = lax.all_gather(away, "core", axis=0, tiled=False)
    own, rest_tail, rest = call(
        pair_kernel,
        (home, got),
        (sds((T, 4, 4, C), F32), sds((OVMAX, 4, 4, C), BF16), sds((T - OVMAX, 4, 4, C), BF16)),
        cost=cost(1),
    )
    swap = [(0, 1), (1, 0)]
    rest_tail = lax.ppermute(rest_tail, "yl", swap)
    rest = lax.ppermute(rest, "yl", swap)
    tail = call(tail_kernel, (own, rest_tail, source, vec), sds((OVMAX, 4, 4, C), BF16), cost=cost(1))
    tiles = lax.axis_size(TILE)
    received = lax.ppermute(tail, TILE, [(i, i + 1) for i in range(tiles - 1)])
    out = call(blend_kernel, (own, rest, tail, source, vec, shared, received), sds((T, 4, 4, C), BF16), cost=cost(1))
    return out[None]


def solution(mesh):
    wide = Mesh(mesh.devices.reshape(8, 4, 4, 2, 2), ("z", "yh", "x", "yl", "core"))
    image = P(TILE, None, None, COL, None)
    kernel = P(None, None, None, COL, None)
    in_specs = (image, P(TILE), P(), P(), kernel, P(), P(), kernel, P())
    return jax.shard_map(block, mesh=wide, in_specs=in_specs, out_specs=image, check_vma=False)
```
